32 devices in a mesh: seq: 32 (over z, y, x, core), head: 1.
Axes of the slice: x: 2, y: 2, z: 4, core: 2. Of those that a mesh axis runs over, the one named last changes fastest.
Arguments:
- hidden: bfloat16 [4096, 1024], P('seq'), may hold values from -6 to 6
- query_weight: bfloat16 [1024, 512], P(None, 'head'), may hold values from -0.1875 to 0.1875
- key_weight: bfloat16 [1024, 512], P(None, 'head'), may hold values from -0.1875 to 0.1875
- values: bfloat16 [4096, 512], P('seq', 'head'), may hold values from -6 to 6
- grad_out: bfloat16 [4096, 512], P('seq', 'head'), may hold values from -6 to 6
- random_feats: float32 [8, 64, 256], P('head'), may hold values from -4 to 4
Outputs:
- grad_hidden: float32 [4096, 1024], P('seq')
- grad_values: bfloat16 [4096, 512], P('seq', 'head')
- grad_query_weight: float32 [1024, 512], P('seq', 'head')
- grad_key_weight: float32 [1024, 512], P('seq', 'head')
The draws below stay inside these ranges and needn't reach their ends.
All inputs are finite; a program needn't handle non-finite values.
Results may differ from the reference program's by a relative error of at most 0.0038.
Values sent between devices are 32-bit elements; how exact they have to be, the bound alone decides.
A program may use at most 64 MiB of HBM per device.

```python
import jax
import jax.numpy as jnp
from jax import lax

D = 1024
HEADS = 8
DH = 64
M = 256
E = 512
S = 4096


def raised(drawn, own_key, source, target, blocks, factor):
    owner, partner = [(jnp.arange(drawn.shape[dim]) // (drawn.shape[dim] // blocks)).reshape([-1 if axis == dim else 1 for axis in range(drawn.ndim)]) for dim in (source, target)]
    chosen = jax.random.permutation(own_key, blocks)[partner]
    strong = (owner == chosen) | (owner == (partner + blocks // 2) % blocks)
    return jnp.where(strong, factor * drawn, drawn)


def steps_of(key, dims, split, least, top_value):
    def one(position, blocks):
        steps = jax.random.uniform(jax.random.fold_in(jax.random.fold_in(key, 6), position), (blocks,), jnp.float32, least / len(split), top_value / len(split))
        return jnp.repeat(jnp.exp(steps), dims[position] // blocks).reshape((-1,) + (1,) * (len(dims) - position - 1))

    gain = one(*split[0])
    for cut in split[1:]:
        gain = gain * one(*cut)
    return gain


def normal_values(own_key, extent, spread, reach, cuts=(), kind=jnp.bfloat16):
    result = jax.random.normal(own_key, extent, jnp.float32) * spread
    if len(cuts) > 0:
        result = steps_of(own_key, extent, cuts, -0.22, 0.18) * result
    return jnp.clip(result, min=-reach, max=reach).astype(kind)


def noise_with(key, dims, deviation, limit, split, heavy, dtype=jnp.bfloat16):
    entries = deviation * jax.random.normal(key, dims, jnp.float32)
    if split:
        entries = entries * steps_of(key, dims, split, -0.22, 0.18)
    return jnp.clip(raised(entries, jax.random.fold_in(key, 3), *heavy), -limit, limit).astype(dtype)


def setup_inputs(seed: int = 0) -> dict:
    key_of = jax.random.split(jax.random.key(seed), 7)
    return {
        "hidden": noise_with(key_of[0], (S, D), 1.0, 6.0, ((0, 32),), (0, 1, 32, 2.75)),
        "query_weight": normal_values(key_of[1], (D, E), D ** -0.5, 0.1875),
        "key_weight": normal_values(key_of[2], (D, E), D ** -0.5, 0.1875),
        "values": normal_values(key_of[3], (S, E), 1.0, 6.0, ((0, 32),)),
        "grad_out": normal_values(key_of[4], (S, E), 1.0, 6.0, ((0, 32),)),
        "random_feats": normal_values(key_of[5], (HEADS, DH, M), 1.0, 4.0, (), jnp.float32),
    }


HIGH = lax.Precision.HIGHEST

def features(rows, table):
    logits = jnp.dot(rows, table, precision=HIGH)
    half_norm = 0.5 * lax.optimization_barrier(jnp.sum(rows * rows, axis=1, keepdims=True))
    return jnp.exp(logits - half_norm) * M ** (-0.5)

def feature_grad(rows, feats, grads, table, feature_scale):
    weighted = feats * grads
    back = jnp.dot(weighted, table.T, precision=HIGH)
    return (back - rows * lax.optimization_barrier(jnp.sum(weighted, axis=1, keepdims=True))) * feature_scale

def one_head(packed):
    query_rows, key_rows, value_rows, upstream, table = packed
    feature_scale = DH ** (-0.25)
    query_feats = features(query_rows, table)
    key_feats = features(key_rows, table)
    value_state = jnp.dot(value_rows.T, key_feats, precision=HIGH)
    normalizer = lax.optimization_barrier(jnp.sum(key_feats, axis=0))
    numerator = jnp.dot(query_feats, value_state.T, precision=HIGH)
    denominator = jnp.dot(query_feats, normalizer, precision=HIGH)
    attended = numerator / denominator[:, None]
    grad_numer = upstream / denominator[:, None]
    grad_denom = -lax.optimization_barrier(jnp.sum(upstream * attended, axis=1)) / denominator
    grad_qfeat = jnp.dot(grad_numer, value_state, precision=HIGH) + grad_denom[:, None] * normalizer[None, :]
    grad_state = jnp.dot(grad_numer.T, query_feats, precision=HIGH)
    grad_normal = jnp.dot(grad_denom, query_feats, precision=HIGH)
    grad_kfeat = jnp.dot(value_rows, grad_state, precision=HIGH) + grad_normal[None, :]
    grad_value = jnp.dot(key_feats, grad_state.T, precision=HIGH)
    grad_query = feature_grad(query_rows, query_feats, grad_qfeat, table, feature_scale)
    grad_key = feature_grad(key_rows, key_feats, grad_kfeat, table, feature_scale)
    return (grad_query, grad_key, grad_value)

def split_heads(matrix):
    return matrix.reshape(S, HEADS, DH).transpose(1, 0, 2)

def join_heads(stacked):
    return stacked.transpose(1, 0, 2).reshape(S, E)

def reference(hidden, query_weight, key_weight, values, grad_out, random_feats):
    hidden_f = hidden.astype(jnp.float32)
    wq_f = query_weight.astype(jnp.float32)
    wk_f = key_weight.astype(jnp.float32)
    feature_scale = DH ** (-0.25)
    query_all = jnp.dot(hidden_f, wq_f, precision=HIGH) * feature_scale
    key_all = jnp.dot(hidden_f, wk_f, precision=HIGH) * feature_scale
    grad_query, grad_key, grad_value = lax.map(one_head, (split_heads(query_all), split_heads(key_all), split_heads(values.astype(jnp.float32)), split_heads(grad_out.astype(jnp.float32)), random_feats))
    dq_round = join_heads(grad_query).astype(jnp.bfloat16).astype(jnp.float32)
    dk_round = join_heads(grad_key).astype(jnp.bfloat16).astype(jnp.float32)
    grad_values = join_heads(grad_value).astype(jnp.bfloat16)
    grad_query_weight = jnp.dot(hidden_f.T, dq_round, precision=HIGH)
    grad_key_weight = jnp.dot(hidden_f.T, dk_round, precision=HIGH)
    grad_hidden = jnp.dot(dq_round, wq_f.T, precision=HIGH) + jnp.dot(dk_round, wk_f.T, precision=HIGH)
    return (grad_hidden, grad_values, grad_query_weight, grad_key_weight)
```

```python
import functools

import jax
import jax.numpy as jnp
from jax import lax
from jax.experimental import pallas as pl
from jax.experimental.pallas import tpu as pltpu
from jax.sharding import PartitionSpec as P

F32, BF16 = jnp.float32, jnp.bfloat16
LANES = 128
MESH = pl.DeviceIdType.MESH


def flipped(index, mask, stride=1):
    out, b = index, 0
    while mask >> b:
        if (mask >> b) & 1:
            bit = (index // (stride * 2**b)) % 2
            out = out + (1 - 2 * bit) * (stride * 2**b)
        b += 1
    return out


def radices(count):
    out = []
    while count > 1:
        out.append(4 if count % 4 == 0 else 2)
        count //= out[-1]
    return out


def dot(a, b):
    return jnp.dot(a, b, preferred_element_type=F32)


def dot_t(a, b):
    return lax.dot_general(a, b, (((1,), (1,)), ((), ())), preferred_element_type=F32)


def halves(x):
    high = x.astype(BF16)
    return high, (x - high.astype(F32)).astype(BF16)


def swap(x):
    return pltpu.roll(x, LANES // 2, 1)


def remote(src, dst, send_sem, recv_sem, peer):
    return pltpu.make_async_remote_copy(
        src_ref=src, dst_ref=dst, send_sem=send_sem, recv_sem=recv_sem,
        device_id={"seq": peer}, device_id_type=MESH,
    )


def kernel(
    n, hid, wq, wk, val, gout, rf, o_hid, o_val, o_gq, o_gk,
    hid_f, hid_r, kv_s, kv_a, qg_s, qg_a, rfs, rbs, feat_k, feat_q, bwd_x,
    ar_s, ar_r, pq_s, pq_r, pk_s, pk_r, dq_p, dk_p, gv_p, dq_a, dk_a, gv_a, gw_s, gw_r,
    a2a_ss, a2a_rs, ar_ss, ar_rs, pair_ss, pair_rs, back_ss, back_rs, gw_ss, gw_rs, loc_s,
):
    groups, head_dim, feats = rf.shape
    toks, width = hid.shape
    half = width // 2
    pairs = groups // 2
    scale = head_dim ** (-0.25)
    norm = feats ** (-0.5)
    me = lax.axis_index("seq")
    mine = me % groups
    core = me % 2
    pair = mine // 2
    first = core == 0
    phases = radices(n // groups)

    barrier = pltpu.get_barrier_semaphore()

    def greet(step, carry):
        pl.semaphore_signal(
            barrier, inc=1, device_id={"seq": (me + step) % n}, device_id_type=MESH
        )
        return carry

    lax.fori_loop(1, n, greet, 0)

    def low(shape):
        return lax.broadcasted_iota(jnp.int32, shape, 1) < head_dim

    def pack(proj, other, out):
        for p in range(pairs):
            a = proj[:, p * LANES : (p + 1) * LANES]
            b = other[:, p * LANES : (p + 1) * LANES].astype(F32)
            mask = low(a.shape)
            out[2 * p] = jnp.where(mask, a, swap(b))
            out[2 * p + 1] = jnp.where(mask, swap(a), b)

    def scatter(which, sent, got):
        copies = []
        for m in range(1, groups):
            to = flipped(me, m)
            copy = remote(
                sent.at[to % groups], got.at[m], a2a_ss.at[which, m], a2a_rs.at[which, m], to
            )
            copy.start()
            copies.append(copy)
        got[0] = sent[mine]
        return copies

    pack(dot(hid[...], wk[...]) * scale, val[...], kv_s)
    pl.semaphore_wait(barrier, n - 1)
    kv_copies = scatter(0, kv_s, kv_a)
    pack(dot(hid[...], wq[...]) * scale, gout[...], qg_s)
    qg_copies = scatter(1, qg_s, qg_a)
    hid_f[0] = hid[:, :half].astype(F32)
    hid_f[1] = hid[:, half:].astype(F32)
    hid_copies = []
    for m in range(1, groups):
        to = flipped(me, m)
        copy = remote(hid_f.at[to % 2], hid_r.at[m - 1], a2a_ss.at[2, m], a2a_rs.at[2, m], to)
        copy.start()
        hid_copies.append(copy)

    rf_high, rf_low = halves(rf[mine])
    rfs[...] = jnp.concatenate([rf_high, rf_high, rf_low, rf_low], axis=0)
    rbs[...] = jnp.concatenate([rf_high, rf_low], axis=0)

    def features(x):
        rows = jnp.where(low(x.shape), x, 0.0)
        high = rows.astype(BF16).astype(F32)
        both = (high + swap(rows - high)).astype(BF16)
        logits = dot(jnp.concatenate([both, both], axis=1), rfs[...])
        return jnp.exp(logits - 0.5 * jnp.sum(rows * rows, axis=1, keepdims=True)) * norm

    def chunk(ref, c):
        return ref[2 * c : 2 * c + 2].reshape(2 * toks, ref.shape[2])

    def all_reduce(which, total):
        stride, slot = groups, 0
        for f, radix in enumerate(phases):
            ar_s[which, f] = total
            copies = []
            for d in range(1, radix):
                copy = remote(
                    ar_s.at[which, f], ar_r.at[which, f, d - 1],
                    ar_ss.at[which, f, d], ar_rs.at[which, f, d], flipped(me, d, stride),
                )
                copy.start()
                copies.append(copy)
            yield
            for d, copy in enumerate(copies):
                copy.wait()
                total = total + ar_r[which, f, d]
            stride *= radix
        summed = jnp.concatenate(
            [jnp.broadcast_to(total[7:8], (head_dim, feats)), total[8:]], axis=0
        )
        yield halves(summed)

    def finish(steps):
        for got in steps:
            if got is not None:
                return got

    lead = head_dim - 8

    total = jnp.zeros((LANES, feats), F32)
    for c in range(pairs):
        for m in (2 * c, 2 * c + 1):
            if m > 0:
                kv_copies[m - 1].wait()
        x = chunk(kv_a, c)
        b = features(x)
        feat_k[c] = b
        high, rest = halves(b)
        ones = jnp.where(low(x.shape), 1.0, x).T.astype(BF16)
        total = total + dot(ones, high) + dot(ones, rest)
    reduce_k = all_reduce(0, total[lead:])
    next(reduce_k)

    for c in range(pairs):
        for m in (2 * c, 2 * c + 1):
            if m > 0:
                qg_copies[m - 1].wait()
        feat_q[c] = features(chunk(qg_a, c))

    st_high, st_low = finish(reduce_k)
    st_both = jnp.concatenate([st_high, st_low], axis=0)
    total = jnp.zeros((LANES, feats), F32)
    for c in range(pairs):
        x = chunk(qg_a, c)
        high, rest = halves(feat_q[c])
        nd = dot_t(high, st_both)
        nd = nd[:, :LANES] + nd[:, LANES:] + dot_t(rest, st_high)
        mask = low(nd.shape)
        den = jnp.where(mask, nd, swap(nd))
        upstream = jnp.where(mask, 0.0, x) / den
        grad_den = -jnp.sum(upstream * nd / den, axis=1, keepdims=True)
        lane = lax.broadcasted_iota(jnp.int32, nd.shape, 1)
        xg = jnp.where(lane == head_dim - 1, grad_den, upstream)
        bwd_x[c] = xg
        turned_high, turned_low = halves(xg.T)
        total = total + dot(turned_high, high) + dot(turned_low, high) + dot(turned_high, rest)
    reduce_q = all_reduce(1, total[lead:])
    next(reduce_q)

    def feature_grad(x, weighted):
        high, rest = halves(weighted)
        back = dot_t(high, rbs[...]) + dot_t(rest, rbs[...])
        back = back + swap(back)
        out = (back - x * jnp.sum(weighted, axis=1, keepdims=True)) * scale
        return jnp.where(low(x.shape), out.astype(BF16).astype(F32), 0.0)

    for c in range(pairs):
        x = chunk(qg_a, c)
        high, rest = halves(bwd_x[c])
        grads = dot(
            jnp.concatenate([high, rest], axis=1), jnp.concatenate([st_high, st_high], axis=0)
        ) + dot(high, st_low)
        out = feature_grad(x, feat_q[c] * grads)
        placed = jnp.where(first, out, swap(out))
        pq_s[2 * c] = placed[:toks]
        pq_s[2 * c + 1] = placed[toks:]
    partner = flipped(me, 1)
    pq_copy = remote(pq_s, pq_r, pair_ss.at[0], pair_rs.at[0], partner)
    pq_copy.start()

    def give_back(which, sent, got):
        copies = []
        for m in range(2, groups, 2):
            copy = remote(
                sent.at[m], got.at[pair], back_ss.at[which, m], back_rs.at[which, m], flipped(me, m)
            )
            copy.start()
            copies.append(copy)
        got[pair] = sent[0]
        return copies

    pq_copy.wait()
    for m in range(groups):
        dq_p[m] = pq_s[m] + pq_r[m ^ 1]
    dq_copies = give_back(0, dq_p, dq_a)

    gs_high, gs_low = finish(reduce_q)
    gs_both = jnp.concatenate([gs_high, gs_low], axis=0)
    for c in range(pairs):
        x = chunk(kv_a, c)
        mask = low(x.shape)
        lane = lax.broadcasted_iota(jnp.int32, x.shape, 1)
        xv = jnp.where(mask, jnp.where(lane == head_dim - 1, 1.0, 0.0), x).astype(BF16)
        b = feat_k[c]
        grads = dot(jnp.concatenate([xv, xv], axis=1), gs_both)
        out = feature_grad(x, b * grads)
        high, rest = halves(b)
        gv = dot_t(high, gs_both)
        gv = gv[:, :LANES] + gv[:, LANES:] + dot_t(rest, gs_high)
        packed = jnp.where(mask, out, gv)
        pk_s[2 * c] = packed[:toks]
        pk_s[2 * c + 1] = packed[toks:]
    pk_copy = remote(pk_s, pk_r, pair_ss.at[1], pair_rs.at[1], partner)
    pk_copy.start()

    for copy in hid_copies:
        copy.wait()

    owner_half = me // (n // 2)

    def weight_sends(which, grads_p):
        total = jnp.zeros((LANES, half), F32)
        for m in range(groups):
            rows = hid_f[core] if m == 0 else hid_r[m - 1]
            total = total + dot(grads_p[m].T.astype(BF16), rows.astype(BF16))
        gw_s[which] = total.T.reshape(gw_s.shape[1:])

        def start(i, carry):
            to = core * (n // 2) + i

            @pl.when(to != me)
            def _():
                remote(
                    gw_s.at[which, i], gw_r.at[which, me // 2],
                    gw_ss.at[which, i], gw_rs.at[which, me // 2], to,
                ).start()

            @pl.when(to == me)
            def _():
                pltpu.make_async_copy(
                    gw_s.at[which, i], gw_r.at[which, me // 2], loc_s.at[which]
                ).start()

            return carry

        lax.fori_loop(0, n // 2, start, 0)

    def weight_waits(which, out):
        def wait(i, carry):
            to = core * (n // 2) + i
            source = 2 * i + owner_half
            here = remote(
                gw_s.at[which, i], gw_r.at[which, i], gw_ss.at[which, i], gw_rs.at[which, i], partner
            )

            @pl.when(to != me)
            def _():
                here.wait_send()

            @pl.when(to == me)
            def _():
                pltpu.make_async_copy(
                    gw_s.at[which, i], gw_r.at[which, me // 2], loc_s.at[which]
                ).wait()

            @pl.when(source != me)
            def _():
                here.wait_recv()

            return carry

        lax.fori_loop(0, n // 2, wait, 0)
        for p in range(pairs):
            total = gw_r[which, p]
            for i in range(p + pairs, n // 2, pairs):
                total = total + gw_r[which, i]
            out[:, p * LANES : (p + 1) * LANES] = total

    weight_sends(0, dq_p)

    pk_copy.wait()
    for m in range(groups):
        own, theirs = pk_s[m], pk_r[m ^ 1]
        one = jnp.where(first, own, theirs)
        two = jnp.where(first, theirs, own)
        mask = low(own.shape)
        dk_p[m] = jnp.where(mask, one, swap(two))
        gv_p[m] = jnp.where(mask, swap(one), two)
    weight_sends(1, dk_p)
    dk_copies = give_back(1, dk_p, dk_a)
    gv_copies = give_back(2, gv_p, gv_a)

    def joined(ref):
        return jnp.concatenate([ref[p] for p in range(pairs)], axis=1).astype(BF16)

    for copy in dq_copies:
        copy.wait()
    for copy in dk_copies:
        copy.wait()
    o_hid[...] = dot_t(joined(dq_a), wq[...]) + dot_t(joined(dk_a), wk[...])
    for copy in gv_copies:
        copy.wait()
    o_val[...] = joined(gv_a)
    weight_waits(0, o_gq)
    weight_waits(1, o_gk)


def shards(n, hidden, query_weight, key_weight, values, grad_out, random_feats):
    toks, width = hidden.shape
    groups, head_dim, feats = random_feats.shape
    cols = groups * head_dim
    pairs = groups // 2
    block = width // n
    phases = len(radices(n // groups))
    rows = head_dim + 8
    tok_block = (groups, toks, LANES)
    scratch = [
        pltpu.VMEM((2, toks, width // 2), F32),
        pltpu.VMEM((groups - 1, toks, width // 2), F32),
        pltpu.VMEM(tok_block, F32),
        pltpu.VMEM(tok_block, F32),
        pltpu.VMEM(tok_block, F32),
        pltpu.VMEM(tok_block, F32),
        pltpu.VMEM((4 * head_dim, feats), BF16),
        pltpu.VMEM((2 * head_dim, feats), BF16),
        pltpu.VMEM((pairs, 2 * toks, feats), F32),
        pltpu.VMEM((pairs, 2 * toks, feats), F32),
        pltpu.VMEM((pairs, 2 * toks, LANES), F32),
        pltpu.VMEM((2, phases, rows, feats), F32),
        pltpu.VMEM((2, phases, 3, rows, feats), F32),
        pltpu.VMEM(tok_block, F32),
        pltpu.VMEM(tok_block, F32),
        pltpu.VMEM(tok_block, F32),
        pltpu.VMEM(tok_block, F32),
        pltpu.VMEM(tok_block, F32),
        pltpu.VMEM(tok_block, F32),
        pltpu.VMEM(tok_block, F32),
        pltpu.VMEM((pairs, toks, LANES), F32),
        pltpu.VMEM((pairs, toks, LANES), F32),
        pltpu.VMEM((pairs, toks, LANES), F32),
        pltpu.VMEM((2, n // 2, block, LANES), F32),
        pltpu.VMEM((2, n // 2, block, LANES), F32),
        pltpu.SemaphoreType.DMA((3, groups)),
        pltpu.SemaphoreType.DMA((3, groups)),
        pltpu.SemaphoreType.DMA((2, phases, 4)),
        pltpu.SemaphoreType.DMA((2, phases, 4)),
        pltpu.SemaphoreType.DMA((2,)),
        pltpu.SemaphoreType.DMA((2,)),
        pltpu.SemaphoreType.DMA((3, groups)),
        pltpu.SemaphoreType.DMA((3, groups)),
        pltpu.SemaphoreType.DMA((2, n // 2)),
        pltpu.SemaphoreType.DMA((2, n // 2)),
        pltpu.SemaphoreType.DMA((2,)),
    ]
    vmem = pl.BlockSpec(memory_space=pltpu.VMEM)
    return pl.pallas_call(
        functools.partial(kernel, n),
        out_shape=(
            jax.ShapeDtypeStruct((toks, width), F32),
            jax.ShapeDtypeStruct((toks, cols), BF16),
            jax.ShapeDtypeStruct((block, cols), F32),
            jax.ShapeDtypeStruct((block, cols), F32),
        ),
        in_specs=[vmem] * 6,
        out_specs=(vmem,) * 4,
        scratch_shapes=scratch,
        compiler_params=pltpu.CompilerParams(
            collective_id=0, has_side_effects=True, vmem_limit_bytes=56 * 2**20
        ),
        name="backward",
    )(hidden, query_weight, key_weight, values, grad_out, random_feats)


def solution(mesh):
    placed = (
        P("seq", None),
        P(None, "head"),
        P(None, "head"),
        P("seq", "head"),
        P("seq", "head"),
        P("head", None, None),
    )

    def local(*args):
        out = shards(mesh.shape["seq"], *args)
        if mesh.shape["head"] == 1:
            return out
        return (lax.psum(out[0], "head"),) + tuple(out[1:])

    return jax.shard_map(
        local,
        mesh=mesh,
        in_specs=placed,
        out_specs=(P("seq", None), P("seq", "head"), P("seq", "head"), P("seq", "head")),
        check_vma=False,
    )
```

```python
import functools

import jax
import jax.numpy as jnp
from jax import lax
from jax.experimental import pallas as pl
from jax.experimental.pallas import tpu as pltpu
from jax.sharding import PartitionSpec as P

F32, BF16 = jnp.float32, jnp.bfloat16
LANES = 128
MESH = pl.DeviceIdType.MESH


def flipped(index, mask, stride=1):
    out, b = index, 0
    while mask >> b:
        if (mask >> b) & 1:
            bit = (index // (stride * 2**b)) % 2
            out = out + (1 - 2 * bit) * (stride * 2**b)
        b += 1
    return out


def radices(count):
    out = []
    while count > 1:
        out.append(4 if count % 4 == 0 else 2)
        count //= out[-1]
    return out


def dot(a, b):
    return jnp.dot(a, b, preferred_element_type=F32)


def dot_t(a, b):
    return lax.dot_general(a, b, (((1,), (1,)), ((), ())), preferred_element_type=F32)


def halves(x):
    high = x.astype(BF16)
    return high, (x - high.astype(F32)).astype(BF16)


def swap(x):
    return pltpu.roll(x, LANES // 2, 1)


def remote(src, dst, send_sem, recv_sem, peer):
    return pltpu.make_async_remote_copy(
        src_ref=src, dst_ref=dst, send_sem=send_sem, recv_sem=recv_sem,
        device_id={"seq": peer}, device_id_type=MESH,
    )


def kernel(
    n, hid_h, wq_h, wk_h, val_h, gout_h, rf_h, o_hid, o_val, o_gq, o_gk,
    hid, wq, wk, val, gout, rf,
    hid_f, hid_r, kv_s, kv_a, qg_s, qg_a, rfs, rbs, feat_k, feat_q, bwd_x,
    ar_s, ar_r, pq_s, pq_r, pk_s, pk_r, dq_p, dk_p, gv_p, turned, dq_a, dk_a, gv_a, gw_s, gw_r,
    in_ss, a2a_ss, a2a_rs, hid_ss, hid_rs, ar_ss, ar_rs, pair_ss, pair_rs, back_ss, back_rs,
    gw_ss, gw_rs, loc_s,
):
    groups, head_dim, feats = rf.shape
    toks, width = hid.shape
    half = width // 2
    parts = half // LANES
    block = gw_s.shape[2]
    per = LANES // block
    pairs = groups // 2
    scale = head_dim ** (-0.25)
    norm = feats ** (-0.5)
    me = lax.axis_index("seq")
    mine = me % groups
    core = me % 2
    pair = mine // 2
    first = core == 0
    phases = radices(n // groups)
    partner = flipped(me, 1)

    barrier = pltpu.get_barrier_semaphore()

    def greet(step, carry):
        pl.semaphore_signal(
            barrier, inc=1, device_id={"seq": (me + step) % n}, device_id_type=MESH
        )
        return carry

    lax.fori_loop(1, n, greet, 0)
    loads = []
    for i, (src, dst) in enumerate(
        [(hid_h, hid), (wk_h, wk), (val_h, val), (wq_h, wq), (gout_h, gout), (rf_h, rf)]
    ):
        loads.append(pltpu.make_async_copy(src, dst, in_ss.at[i]))
        loads[-1].start()

    def low(shape):
        return lax.broadcasted_iota(jnp.int32, shape, 1) < head_dim

    def pack(proj, other, out):
        for p in range(pairs):
            a = proj[:, p * LANES : (p + 1) * LANES]
            b = other[:, p * LANES : (p + 1) * LANES].astype(F32)
            mask = low(a.shape)
            out[2 * p] = jnp.where(mask, a, swap(b))
            out[2 * p + 1] = jnp.where(mask, swap(a), b)

    def scatter(which, sent, got):
        copies = []
        for m in range(1, groups):
            to = flipped(me, m)
            copy = remote(
                sent.at[to % groups], got.at[m], a2a_ss.at[which, m], a2a_rs.at[which, m], to
            )
            copy.start()
            copies.append(copy)
        got[0] = sent[mine]
        return copies

    for load in loads[:3]:
        load.wait()
    pack(dot(hid[...], wk[...]) * scale, val[...], kv_s)
    pl.semaphore_wait(barrier, n - 1)
    kv_copies = scatter(0, kv_s, kv_a)
    for load in loads[3:5]:
        load.wait()
    pack(dot(hid[...], wq[...]) * scale, gout[...], qg_s)
    qg_copies = scatter(1, qg_s, qg_a)

    for h in range(2):
        for q in range(parts):
            spot = h * half + q * LANES
            hid_f[h, q] = hid[:, spot : spot + LANES].astype(F32)

    def hidden_copy(q, m):
        if m & 6 == 6:
            via, hop = (2, 4) if m == 6 else (5, 2)
            return remote(
                hid_r.at[q, via], hid_r.at[q, m], hid_ss.at[q, m], hid_rs.at[q, m], flipped(me, hop)
            )
        to = flipped(me, m)
        return remote(
            hid_f.at[to % 2, q], hid_r.at[q, m], hid_ss.at[q, m], hid_rs.at[q, m], to
        )

    relayed = [m for m in range(1, groups) if m & 6 == 6 and m < 8]
    direct = [m for m in range(1, groups) if m not in relayed]
    hidden = {(q, m): hidden_copy(q, m) for q in range(parts) for m in range(1, groups)}

    def send_hidden(q):
        if q < parts:
            for m in direct:
                hidden[q, m].start()
            hid_r[q, 0] = hid_f[core, q]

    ahead = 2
    for q in range(ahead):
        send_hidden(q)

    def relay(q):
        if q >= parts:
            return
        for m in relayed:
            hidden[q, 2 if m == 6 else 5].wait_recv()
            hidden[q, m].start()
        send_hidden(q + ahead)

    def hidden_rows(q):
        for m in range(1, groups):
            if not (relayed and m in (2, 5)):
                hidden[q, m].wait_recv()
        return hid_r[q].reshape(groups * toks, LANES).astype(BF16)

    loads[5].wait()
    rf_high, rf_low = halves(rf[mine])
    rfs[...] = jnp.concatenate([rf_high, rf_high, rf_low, rf_low], axis=0)
    rbs[...] = jnp.concatenate([rf_high, rf_low], axis=0)

    def features(x):
        rows = jnp.where(low(x.shape), x, 0.0)
        high = rows.astype(BF16).astype(F32)
        both = (high + swap(rows - high)).astype(BF16)
        logits = dot(jnp.concatenate([both, both], axis=1), rfs[...])
        return jnp.exp(logits - 0.5 * jnp.sum(rows * rows, axis=1, keepdims=True)) * norm

    def chunk(ref, c):
        return ref[2 * c : 2 * c + 2].reshape(2 * toks, ref.shape[2])

    def all_reduce(which, total):
        stride = groups
        for f, radix in enumerate(phases):
            ar_s[which, f] = total
            copies = []
            for d in range(1, radix):
                copy = remote(
                    ar_s.at[which, f], ar_r.at[which, f, d - 1],
                    ar_ss.at[which, f, d], ar_rs.at[which, f, d], flipped(me, d, stride),
                )
                copy.start()
                copies.append(copy)
            yield
            for d, copy in enumerate(copies):
                copy.wait()
                total = total + ar_r[which, f, d]
            stride *= radix
        summed = jnp.concatenate(
            [jnp.broadcast_to(total[7:8], (head_dim, feats)), total[8:]], axis=0
        )
        yield halves(summed)

    def finish(steps):
        for got in steps:
            if got is not None:
                return got

    lead = head_dim - 8

    total = jnp.zeros((LANES, feats), F32)
    for c in range(pairs):
        for m in (2 * c, 2 * c + 1):
            if m > 0:
                kv_copies[m - 1].wait()
        x = chunk(kv_a, c)
        b = features(x)
        feat_k[c] = b
        high, rest = halves(b)
        ones = jnp.where(low(x.shape), 1.0, x).T.astype(BF16)
        total = total + dot(ones, high) + dot(ones, rest)
    reduce_k = all_reduce(0, total[lead:])
    next(reduce_k)

    for c in range(pairs):
        for m in (2 * c, 2 * c + 1):
            if m > 0:
                qg_copies[m - 1].wait()
        feat_q[c] = features(chunk(qg_a, c))

    st_high, st_low = finish(reduce_k)
    st_both = jnp.concatenate([st_high, st_low], axis=0)
    total = jnp.zeros((LANES, feats), F32)
    for c in range(pairs):
        x = chunk(qg_a, c)
        high, rest = halves(feat_q[c])
        nd = dot_t(high, st_both)
        nd = nd[:, :LANES] + nd[:, LANES:] + dot_t(rest, st_high)
        mask = low(nd.shape)
        den = jnp.where(mask, nd, swap(nd))
        upstream = jnp.where(mask, 0.0, x) / den
        grad_den = -jnp.sum(upstream * nd / den, axis=1, keepdims=True)
        lane = lax.broadcasted_iota(jnp.int32, nd.shape, 1)
        xg = jnp.where(lane == head_dim - 1, grad_den, upstream)
        bwd_x[c] = xg
        turned_high, turned_low = halves(xg.T)
        total = total + dot(turned_high, high) + dot(turned_low, high) + dot(turned_high, rest)
    reduce_q = all_reduce(1, total[lead:])
    next(reduce_q)
    relay(0)

    def feature_grad(x, weighted):
        high, rest = halves(weighted)
        back = dot_t(high, rbs[...]) + dot_t(rest, rbs[...])
        back = back + swap(back)
        out = (back - x * jnp.sum(weighted, axis=1, keepdims=True)) * scale
        return jnp.where(low(x.shape), out.astype(BF16).astype(F32), 0.0)

    def pair_copy(which, sent, got, c):
        two = pl.ds(2 * c, 2)
        copy = remote(
            sent.at[two], got.at[two], pair_ss.at[which, c], pair_rs.at[which, c], partner
        )
        copy.start()
        return copy

    pq_copies = []
    for c in range(pairs):
        x = chunk(qg_a, c)
        high, rest = halves(bwd_x[c])
        grads = dot(
            jnp.concatenate([high, rest], axis=1), jnp.concatenate([st_high, st_high], axis=0)
        ) + dot(high, st_low)
        out = feature_grad(x, feat_q[c] * grads)
        placed = jnp.where(first, out, swap(out))
        pq_s[2 * c] = placed[:toks]
        pq_s[2 * c + 1] = placed[toks:]
        pq_copies.append(pair_copy(0, pq_s, pq_r, c))

    def give_back(which, sent, got):
        copies = []
        for m in range(2, groups, 2):
            copy = remote(
                sent.at[m], got.at[pair], back_ss.at[which, m], back_rs.at[which, m], flipped(me, m)
            )
            copy.start()
            copies.append(copy)
        got[pair] = sent[0]
        return copies

    relay(1)
    for c in range(pairs):
        pq_copies[c].wait()
        for m in (2 * c, 2 * c + 1):
            both = pq_s[m] + pq_r[m ^ 1]
            dq_p[m] = both
            turned[0, :, m * toks : (m + 1) * toks] = both.T.astype(BF16)

    def weight_part(which, q, rows):
        total = dot(turned[which], rows).T
        gw_s[which, q * per : (q + 1) * per] = total.reshape(per, block, LANES)

    def weight_sends(which, q):
        def start(i, carry):
            to = core * (n // 2) + i

            @pl.when(to != me)
            def _():
                remote(
                    gw_s.at[which, i], gw_r.at[which, me // 2],
                    gw_ss.at[which, i], gw_rs.at[which, me // 2], to,
                ).start()

            @pl.when(to == me)
            def _():
                pltpu.make_async_copy(
                    gw_s.at[which, i], gw_r.at[which, me // 2], loc_s.at[which]
                ).start()

            return carry

        lax.fori_loop(q * per, (q + 1) * per, start, 0)

    weight_part(0, 0, hidden_rows(0))

    gs_high, gs_low = finish(reduce_q)
    weight_sends(0, 0)
    gs_both = jnp.concatenate([gs_high, gs_low], axis=0)
    pk_copies = []
    for c in range(pairs):
        x = chunk(kv_a, c)
        mask = low(x.shape)
        lane = lax.broadcasted_iota(jnp.int32, x.shape, 1)
        xv = jnp.where(mask, jnp.where(lane == head_dim - 1, 1.0, 0.0), x).astype(BF16)
        b = feat_k[c]
        grads = dot(jnp.concatenate([xv, xv], axis=1), gs_both)
        out = feature_grad(x, b * grads)
        high, rest = halves(b)
        gv = dot_t(high, gs_both)
        gv = gv[:, :LANES] + gv[:, LANES:] + dot_t(rest, gs_high)
        packed = jnp.where(mask, out, gv)
        pk_s[2 * c] = packed[:toks]
        pk_s[2 * c + 1] = packed[toks:]
        pk_copies.append(pair_copy(1, pk_s, pk_r, c))
    relay(2)
    weight_part(0, 1, hidden_rows(1))
    weight_sends(0, 1)
    for c in range(pairs):
        pk_copies[c].wait()
        for m in (2 * c, 2 * c + 1):
            own, theirs = pk_s[m], pk_r[m ^ 1]
            one = jnp.where(first, own, theirs)
            two = jnp.where(first, theirs, own)
            mask = low(own.shape)
            both = jnp.where(mask, one, swap(two))
            dk_p[m] = both
            turned[1, :, m * toks : (m + 1) * toks] = both.T.astype(BF16)
            gv_p[m] = jnp.where(mask, swap(one), two)
    for q in range(2):
        weight_part(1, q, hid_r[q].reshape(groups * toks, LANES).astype(BF16))
        weight_sends(1, q)
    for q in range(2, parts):
        relay(q + 1)
        if q == parts - 1:
            dq_copies = give_back(0, dq_p, dq_a)
            dk_copies = give_back(1, dk_p, dk_a)
        rows = hidden_rows(q)
        for which in range(2):
            weight_part(which, q, rows)
            weight_sends(which, q)
    gv_copies = give_back(2, gv_p, gv_a)

    def joined(ref):
        return jnp.concatenate([ref[p] for p in range(pairs)], axis=1).astype(BF16)

    for copy in dq_copies:
        copy.wait()
    o_hid[...] = dot_t(joined(dq_a), wq[...])
    for copy in dk_copies:
        copy.wait()
    o_hid[...] += dot_t(joined(dk_a), wk[...])
    for copy in gv_copies:
        copy.wait()
    o_val[...] = joined(gv_a)

    owner_half = me // (n // 2)

    def weight_wait(which, i):
        to = core * (n // 2) + i
        source = 2 * i + owner_half
        here = remote(
            gw_s.at[which, i], gw_r.at[which, i], gw_ss.at[which, i], gw_rs.at[which, i], partner
        )

        @pl.when(to != me)
        def _():
            here.wait_send()

        @pl.when(to == me)
        def _():
            pltpu.make_async_copy(
                gw_s.at[which, i], gw_r.at[which, me // 2], loc_s.at[which]
            ).wait()

        @pl.when(source != me)
        def _():
            here.wait_recv()

    def wait_both(i, carry):
        weight_wait(0, i)
        weight_wait(1, i)
        return carry

    lax.fori_loop(0, n // 2, wait_both, 0)
    for which, out in ((0, o_gq), (1, o_gk)):
        for p in range(pairs):
            total = gw_r[which, p]
            for i in range(p + pairs, n // 2, pairs):
                total = total + gw_r[which, i]
            out[:, p * LANES : (p + 1) * LANES] = total
    for copy in hidden.values():
        copy.wait_send()


def store(*refs):
    count = len(refs) // 2
    sems = refs[-1]
    copies = [
        pltpu.make_async_copy(refs[i], refs[count + i], sems.at[i]) for i in range(count)
    ]
    for copy in copies:
        copy.start()
    for copy in copies:
        copy.wait()


def shards(n, *args):
    hidden, random_feats = args[0], args[5]
    toks, width = hidden.shape
    groups, head_dim, feats = random_feats.shape
    cols = groups * head_dim
    pairs = groups // 2
    block = width // n
    parts = width // 2 // LANES
    phases = len(radices(n // groups))
    rows = head_dim + 8
    tok_block = (groups, toks, LANES)
    own_block = (pairs, toks, LANES)
    scratch = [pltpu.VMEM(a.shape, a.dtype) for a in args]
    scratch += [
        pltpu.VMEM((2, parts, toks, LANES), F32),
        pltpu.VMEM((parts,) + tok_block, F32),
    ]
    scratch += [pltpu.VMEM(tok_block, F32)] * 4
    scratch += [
        pltpu.VMEM((4 * head_dim, feats), BF16),
        pltpu.VMEM((2 * head_dim, feats), BF16),
        pltpu.VMEM((pairs, 2 * toks, feats), F32),
        pltpu.VMEM((pairs, 2 * toks, feats), F32),
        pltpu.VMEM((pairs, 2 * toks, LANES), F32),
        pltpu.VMEM((2, phases, rows, feats), F32),
        pltpu.VMEM((2, phases, 3, rows, feats), F32),
    ]
    scratch += [pltpu.VMEM(tok_block, F32)] * 7
    scratch += [pltpu.VMEM((2, LANES, groups * toks), BF16)]
    scratch += [pltpu.VMEM(own_block, F32)] * 3
    scratch += [pltpu.VMEM((2, n // 2, block, LANES), F32)] * 2
    scratch += [pltpu.SemaphoreType.DMA((6,))]
    scratch += [pltpu.SemaphoreType.DMA((2, groups))] * 2
    scratch += [pltpu.SemaphoreType.DMA((parts, groups))] * 2
    scratch += [pltpu.SemaphoreType.DMA((2, phases, 4))] * 2
    scratch += [pltpu.SemaphoreType.DMA((2, pairs))] * 2
    scratch += [pltpu.SemaphoreType.DMA((3, groups))] * 2
    scratch += [pltpu.SemaphoreType.DMA((2, n // 2))] * 2
    scratch += [pltpu.SemaphoreType.DMA((2,))]
    vmem = pl.BlockSpec(memory_space=pltpu.VMEM)
    anywhere = pl.BlockSpec(memory_space=pl.ANY)
    shapes = (
        jax.ShapeDtypeStruct((toks, width), F32),
        jax.ShapeDtypeStruct((toks, cols), BF16),
        jax.ShapeDtypeStruct((block, cols), F32),
        jax.ShapeDtypeStruct((block, cols), F32),
    )
    out = pl.pallas_call(
        functools.partial(kernel, n),
        out_shape=tuple(pltpu.VMEM(a.shape, a.dtype) for a in shapes),
        in_specs=[anywhere] * 6,
        out_specs=(vmem,) * 4,
        scratch_shapes=scratch,
        compiler_params=pltpu.CompilerParams(
            collective_id=0, has_side_effects=True, vmem_limit_bytes=56 * 2**20
        ),
        name="backward",
    )(*args)
    return pl.pallas_call(
        store,
        out_shape=shapes,
        in_specs=[vmem] * 4,
        out_specs=(anywhere,) * 4,
        scratch_shapes=[pltpu.SemaphoreType.DMA((4,))],
        name="store",
    )(*[pltpu.with_memory_space_constraint(a, pltpu.VMEM) for a in out])


def solution(mesh):
    placed = (
        P("seq", None),
        P(None, "head"),
        P(None, "head"),
        P("seq", "head"),
        P("seq", "head"),
        P("head", None, None),
    )

    def local(*args):
        out = shards(mesh.shape["seq"], *args)
        if mesh.shape["head"] == 1:
            return out
        return (lax.psum(out[0], "head"),) + tuple(out[1:])

    return jax.shard_map(
        local,
        mesh=mesh,
        in_specs=placed,
        out_specs=(P("seq", None), P("seq", "head"), P("seq", "head"), P("seq", "head")),
        check_vma=False,
    )
```

```python
import functools

import jax
import jax.numpy as jnp
from jax import lax
from jax.experimental import pallas as pl
from jax.experimental.pallas import tpu as pltpu
from jax.sharding import PartitionSpec as P

F32, BF16 = jnp.float32, jnp.bfloat16
LANES = 128
MESH = pl.DeviceIdType.MESH


def flipped(index, mask, stride=1):
    out, b = index, 0
    while mask >> b:
        if (mask >> b) & 1:
            bit = (index // (stride * 2**b)) % 2
            out = out + (1 - 2 * bit) * (stride * 2**b)
        b += 1
    return out


def radices(count):
    out = []
    while count > 1:
        out.append(4 if count % 4 == 0 else 2)
        count //= out[-1]
    return out


def dot(a, b):
    return jnp.dot(a, b, preferred_element_type=F32)


def dot_t(a, b):
    return lax.dot_general(a, b, (((1,), (1,)), ((), ())), preferred_element_type=F32)


def halves(x):
    high = x.astype(BF16)
    return high, (x - high.astype(F32)).astype(BF16)


def swap(x):
    return pltpu.roll(x, LANES // 2, 1)


def settle(ref, sem):
    pltpu.make_async_copy(ref, ref, sem).wait()


def remote(src, dst, send_sem, recv_sem, peer):
    return pltpu.make_async_remote_copy(
        src_ref=src, dst_ref=dst, send_sem=send_sem, recv_sem=recv_sem,
        device_id={"seq": peer}, device_id_type=MESH,
    )


def kernel(
    n, hid_h, wq_h, wk_h, val_h, gout_h, rf_h, o_hid, o_val, o_gq, o_gk,
    hid, wq, wk, val, gout, rf,
    hid_f, hid_r, kv_s, kv_a, qg_s, qg_a, rfs, rbs, feat_k, feat_q, bwd_x,
    ar_s, ar_r, pq_s, pq_r, pk_s, pk_r, dq_p, dk_p, gv_p, turned, dq_a, dk_a, gv_a, gw_s, gw_r,
    in_ss, a2a_ss, a2a_rs, hid_ss, hid_rs, ar_ss, ar_rs, pair_ss, pair_rs, back_ss, back_rs,
    gw_ss, gw_rs,
):
    groups, head_dim, feats = rf.shape
    toks, width = hid.shape
    half = width // 2
    parts = half // LANES
    block = gw_s.shape[2]
    per = LANES // block
    pairs = groups // 2
    scale = head_dim ** (-0.25)
    norm = feats ** (-0.5)
    me = lax.axis_index("seq")
    mine = me % groups
    core = me % 2
    pair = mine // 2
    first = core == 0
    phases = radices(n // groups)
    partner = flipped(me, 1)

    barrier = pltpu.get_barrier_semaphore()

    def greet(step, carry):
        pl.semaphore_signal(
            barrier, inc=1, device_id={"seq": (me + step) % n}, device_id_type=MESH
        )
        return carry

    lax.fori_loop(1, n, greet, 0)
    loads = []
    for i, (src, dst) in enumerate(
        [(hid_h, hid), (wk_h, wk), (val_h, val), (wq_h, wq), (gout_h, gout), (rf_h, rf)]
    ):
        loads.append(pltpu.make_async_copy(src, dst, in_ss.at[i]))
        loads[-1].start()

    def low(shape):
        return lax.broadcasted_iota(jnp.int32, shape, 1) < head_dim

    def pack(proj, other, out):
        for p in range(pairs):
            a = proj[:, p * LANES : (p + 1) * LANES]
            b = other[:, p * LANES : (p + 1) * LANES].astype(F32)
            mask = low(a.shape)
            out[2 * p] = jnp.where(mask, a, swap(b))
            out[2 * p + 1] = jnp.where(mask, swap(a), b)

    def scatter(which, sent, got):
        for m in range(1, groups):
            to = flipped(me, m)
            remote(
                sent.at[to % groups], got.at[m], a2a_ss.at[which], a2a_rs.at[which, m // 2], to
            ).start()
        got[0] = sent[mine]

    def scattered(which, got, c):
        skip = 1 if c == 0 else 0
        settle(got.at[pl.ds(2 * c + skip, 2 - skip)], a2a_rs.at[which, c])

    for load in loads[:3]:
        load.wait()
    pack(dot(hid[...], wk[...]) * scale, val[...], kv_s)
    pl.semaphore_wait(barrier, n - 1)
    scatter(0, kv_s, kv_a)
    for load in loads[3:5]:
        load.wait()
    pack(dot(hid[...], wq[...]) * scale, gout[...], qg_s)
    scatter(1, qg_s, qg_a)

    for h in range(2):
        for q in range(parts):
            spot = h * half + q * LANES
            hid_f[h, q] = hid[:, spot : spot + LANES].astype(F32)

    relayed = [m for m in range(1, groups) if m & 6 == 6 and m < 8]
    direct = [m for m in range(1, groups) if m not in relayed]
    passed_on = [2, 5] if relayed else []
    ahead = 3

    def hidden_start(q, m):
        if m in relayed:
            via, hop = (2, 4) if m == 6 else (5, 2)
            source, to = hid_r.at[q, via], flipped(me, hop)
        else:
            to = flipped(me, m)
            source = hid_f.at[to % 2, q]
        recv = hid_rs.at[q, 1 if m in passed_on else 0]
        remote(source, hid_r.at[q, m], hid_ss.at[0], recv, to).start()

    def send_hidden(q):
        if q < parts:
            for m in passed_on + [m for m in direct if m not in passed_on]:
                hidden_start(q, m)
            hid_r[q, 0] = hid_f[core, q]

    for q in range(ahead):
        send_hidden(q)

    def relay(q):
        if q < parts:
            if passed_on:
                settle(hid_r.at[q, pl.ds(0, len(passed_on))], hid_rs.at[q, 1])
            for m in relayed:
                hidden_start(q, m)
            send_hidden(q + ahead)

    def hidden_rows(q):
        settle(hid_r.at[q, pl.ds(0, groups - 1 - len(passed_on))], hid_rs.at[q, 0])
        return hid_r[q].reshape(groups * toks, LANES).astype(BF16)

    loads[5].wait()
    rf_high, rf_low = halves(rf[mine])
    rfs[...] = jnp.concatenate([rf_high, rf_high, rf_low, rf_low], axis=0)
    rbs[...] = jnp.concatenate([rf_high, rf_low], axis=0)

    def features(x):
        rows = jnp.where(low(x.shape), x, 0.0)
        high = rows.astype(BF16).astype(F32)
        both = (high + swap(rows - high)).astype(BF16)
        logits = dot(jnp.concatenate([both, both], axis=1), rfs[...])
        return jnp.exp(logits - 0.5 * jnp.sum(rows * rows, axis=1, keepdims=True)) * norm

    def chunk(ref, c):
        return ref[2 * c : 2 * c + 2].reshape(2 * toks, ref.shape[2])

    def all_reduce(which, total):
        stride = groups
        for f, radix in enumerate(phases):
            ar_s[which, f] = total
            for d in range(1, radix):
                remote(
                    ar_s.at[which, f], ar_r.at[which, f, d - 1],
                    ar_ss.at[which, f], ar_rs.at[which, f], flipped(me, d, stride),
                ).start()
            yield
            came = ar_r.at[which, f, pl.ds(0, radix - 1)]
            settle(came, ar_rs.at[which, f])
            settle(came, ar_ss.at[which, f])
            for d in range(radix - 1):
                total = total + ar_r[which, f, d]
            stride *= radix
        summed = jnp.concatenate(
            [jnp.broadcast_to(total[7:8], (head_dim, feats)), total[8:]], axis=0
        )
        yield halves(summed)

    def finish(steps):
        for got in steps:
            if got is not None:
                return got

    lead = head_dim - 8

    total = jnp.zeros((LANES, feats), F32)
    for c in range(pairs):
        scattered(0, kv_a, c)
        x = chunk(kv_a, c)
        b = features(x)
        feat_k[c] = b
        high, rest = halves(b)
        ones = jnp.where(low(x.shape), 1.0, x).T.astype(BF16)
        total = total + dot(ones, high) + dot(ones, rest)
    reduce_k = all_reduce(0, total[lead:])
    next(reduce_k)

    for c in range(pairs):
        scattered(1, qg_a, c)
        feat_q[c] = features(chunk(qg_a, c))

    st_high, st_low = finish(reduce_k)
    st_both = jnp.concatenate([st_high, st_low], axis=0)
    total = jnp.zeros((LANES, feats), F32)
    for c in range(pairs):
        x = chunk(qg_a, c)
        high, rest = halves(feat_q[c])
        nd = dot_t(high, st_both)
        nd = nd[:, :LANES] + nd[:, LANES:] + dot_t(rest, st_high)
        mask = low(nd.shape)
        den = jnp.where(mask, nd, swap(nd))
        upstream = jnp.where(mask, 0.0, x) / den
        grad_den = -jnp.sum(upstream * nd / den, axis=1, keepdims=True)
        lane = lax.broadcasted_iota(jnp.int32, nd.shape, 1)
        xg = jnp.where(lane == head_dim - 1, grad_den, upstream)
        bwd_x[c] = xg
        turned_high, turned_low = halves(xg.T)
        total = total + dot(turned_high, high) + dot(turned_low, high) + dot(turned_high, rest)
    reduce_q = all_reduce(1, total[lead:])
    next(reduce_q)
    relay(0)

    def feature_grad(x, weighted):
        high, rest = halves(weighted)
        back = dot_t(high, rbs[...]) + dot_t(rest, rbs[...])
        back = back + swap(back)
        out = (back - x * jnp.sum(weighted, axis=1, keepdims=True)) * scale
        return jnp.where(low(x.shape), out.astype(BF16).astype(F32), 0.0)

    def pair_copy(which, sent, got, c):
        two = pl.ds(2 * c, 2)
        remote(
            sent.at[two], got.at[two], pair_ss.at[which], pair_rs.at[which, c], partner
        ).start()

    def paired(which, got, c):
        settle(got.at[pl.ds(2 * c, 2)], pair_rs.at[which, c])

    for c in range(pairs):
        x = chunk(qg_a, c)
        high, rest = halves(bwd_x[c])
        grads = dot(
            jnp.concatenate([high, rest], axis=1), jnp.concatenate([st_high, st_high], axis=0)
        ) + dot(high, st_low)
        out = feature_grad(x, feat_q[c] * grads)
        placed = jnp.where(first, out, swap(out))
        pq_s[2 * c] = placed[:toks]
        pq_s[2 * c + 1] = placed[toks:]
        pair_copy(0, pq_s, pq_r, c)

    def give_back(which, sent, got):
        for m in range(2, groups, 2):
            remote(
                sent.at[m], got.at[pair], back_ss.at[which], back_rs.at[which], flipped(me, m)
            ).start()
        got[pair] = sent[0]

    def given_back(which, got):
        settle(got.at[pl.ds(0, pairs - 1)], back_rs.at[which])

    relay(1)
    for c in range(pairs):
        paired(0, pq_r, c)
        for m in (2 * c, 2 * c + 1):
            both = pq_s[m] + pq_r[m ^ 1]
            dq_p[m] = both
            turned[0, :, m * toks : (m + 1) * toks] = both.T.astype(BF16)

    def weight_part(which, q, rows):
        total = dot(turned[which], rows).T
        gw_s[which, q * per : (q + 1) * per] = total.reshape(per, block, LANES)

    def weight_sends(which, q):
        def start(i, carry):
            to = core * (n // 2) + i

            @pl.when(to != me)
            def _():
                remote(
                    gw_s.at[which, i], gw_r.at[which, me // 2],
                    gw_ss.at[which], gw_rs.at[which], to,
                ).start()

            @pl.when(to == me)
            def _():
                pltpu.make_async_copy(
                    gw_s.at[which, i], gw_r.at[which, me // 2], gw_rs.at[which]
                ).start()

            return carry

        lax.fori_loop(q * per, (q + 1) * per, start, 0)

    relay(2)
    weight_part(0, 0, hidden_rows(0))

    gs_high, gs_low = finish(reduce_q)
    weight_sends(0, 0)
    gs_both = jnp.concatenate([gs_high, gs_low], axis=0)
    for c in range(pairs):
        x = chunk(kv_a, c)
        mask = low(x.shape)
        lane = lax.broadcasted_iota(jnp.int32, x.shape, 1)
        xv = jnp.where(mask, jnp.where(lane == head_dim - 1, 1.0, 0.0), x).astype(BF16)
        b = feat_k[c]
        grads = dot(jnp.concatenate([xv, xv], axis=1), gs_both)
        out = feature_grad(x, b * grads)
        high, rest = halves(b)
        gv = dot_t(high, gs_both)
        gv = gv[:, :LANES] + gv[:, LANES:] + dot_t(rest, gs_high)
        packed = jnp.where(mask, out, gv)
        pk_s[2 * c] = packed[:toks]
        pk_s[2 * c + 1] = packed[toks:]
        pair_copy(1, pk_s, pk_r, c)
        if c == pairs // 2 - 1:
            relay(3)
    weight_part(0, 1, hidden_rows(1))
    weight_sends(0, 1)
    for c in range(pairs):
        paired(1, pk_r, c)
        for m in (2 * c, 2 * c + 1):
            own, theirs = pk_s[m], pk_r[m ^ 1]
            one = jnp.where(first, own, theirs)
            two = jnp.where(first, theirs, own)
            mask = low(own.shape)
            both = jnp.where(mask, one, swap(two))
            dk_p[m] = both
            turned[1, :, m * toks : (m + 1) * toks] = both.T.astype(BF16)
            gv_p[m] = jnp.where(mask, swap(one), two)
    for q in range(2):
        weight_part(1, q, hid_r[q].reshape(groups * toks, LANES).astype(BF16))
        weight_sends(1, q)
    give_back(0, dq_p, dq_a)
    give_back(1, dk_p, dk_a)
    for q in range(2, parts):
        if q > 2:
            relay(q + 1)
        rows = hidden_rows(q)
        for which in range(2):
            weight_part(which, q, rows)
            weight_sends(which, q)
    give_back(2, gv_p, gv_a)

    def joined(ref):
        return jnp.concatenate([ref[p] for p in range(pairs)], axis=1).astype(BF16)

    given_back(0, dq_a)
    o_hid[...] = dot_t(joined(dq_a), wq[...])
    given_back(1, dk_a)
    o_hid[...] += dot_t(joined(dk_a), wk[...])
    given_back(2, gv_a)
    o_val[...] = joined(gv_a)

    for which in range(2):
        settle(gw_r.at[which], gw_rs.at[which])
    for which, out in ((0, o_gq), (1, o_gk)):
        for p in range(pairs):
            total = gw_r[which, p]
            for i in range(p + pairs, n // 2, pairs):
                total = total + gw_r[which, i]
            out[:, p * LANES : (p + 1) * LANES] = total
    for which in range(2):
        others = kv_a.at[pl.ds(1, groups - 1)]
        settle(others, a2a_ss.at[which])
        settle(pk_s, pair_ss.at[which])
        own_set = me // (n // 2) == core

        @pl.when(own_set)
        def _():
            settle(gw_s.at[which, pl.ds(0, n // 2 - 1)], gw_ss.at[which])

        @pl.when(jnp.logical_not(own_set))
        def _():
            settle(gw_s.at[which], gw_ss.at[which])

    for which in range(3):
        settle(dq_a.at[pl.ds(0, pairs - 1)], back_ss.at[which])
    settle(hid_r.at[:, pl.ds(1, groups - 1)], hid_ss.at[0])


def store(*refs):
    count = len(refs) // 2
    sems = refs[-1]
    copies = [
        pltpu.make_async_copy(refs[i], refs[count + i], sems.at[i]) for i in range(count)
    ]
    for copy in copies:
        copy.start()
    for copy in copies:
        copy.wait()


def shards(n, *args):
    hidden, random_feats = args[0], args[5]
    toks, width = hidden.shape
    groups, head_dim, feats = random_feats.shape
    cols = groups * head_dim
    pairs = groups // 2
    block = width // n
    parts = width // 2 // LANES
    phases = len(radices(n // groups))
    rows = head_dim + 8
    tok_block = (groups, toks, LANES)
    own_block = (pairs, toks, LANES)
    scratch = [pltpu.VMEM(a.shape, a.dtype) for a in args]
    scratch += [
        pltpu.VMEM((2, parts, toks, LANES), F32),
        pltpu.VMEM((parts,) + tok_block, F32),
    ]
    scratch += [pltpu.VMEM(tok_block, F32)] * 4
    scratch += [
        pltpu.VMEM((4 * head_dim, feats), BF16),
        pltpu.VMEM((2 * head_dim, feats), BF16),
        pltpu.VMEM((pairs, 2 * toks, feats), F32),
        pltpu.VMEM((pairs, 2 * toks, feats), F32),
        pltpu.VMEM((pairs, 2 * toks, LANES), F32),
        pltpu.VMEM((2, phases, rows, feats), F32),
        pltpu.VMEM((2, phases, 3, rows, feats), F32),
    ]
    scratch += [pltpu.VMEM(tok_block, F32)] * 7
    scratch += [pltpu.VMEM((2, LANES, groups * toks), BF16)]
    scratch += [pltpu.VMEM(own_block, F32)] * 3
    scratch += [pltpu.VMEM((2, n // 2, block, LANES), F32)] * 2
    for shape in (
        (6,), (2,), (2, pairs), (1,), (parts, 2), (2, phases), (2, phases), (2,), (2, pairs),
        (3,), (3,), (2,), (2,),
    ):
        scratch.append(pltpu.SemaphoreType.DMA(shape))
    vmem = pl.BlockSpec(memory_space=pltpu.VMEM)
    anywhere = pl.BlockSpec(memory_space=pl.ANY)
    shapes = (
        jax.ShapeDtypeStruct((toks, width), F32),
        jax.ShapeDtypeStruct((toks, cols), BF16),
        jax.ShapeDtypeStruct((block, cols), F32),
        jax.ShapeDtypeStruct((block, cols), F32),
    )
    out = pl.pallas_call(
        functools.partial(kernel, n),
        out_shape=tuple(pltpu.VMEM(a.shape, a.dtype) for a in shapes),
        in_specs=[anywhere] * 6,
        out_specs=(vmem,) * 4,
        scratch_shapes=scratch,
        compiler_params=pltpu.CompilerParams(
            collective_id=0, has_side_effects=True, vmem_limit_bytes=56 * 2**20
        ),
        name="backward",
    )(*args)
    return pl.pallas_call(
        store,
        out_shape=shapes,
        in_specs=[vmem] * 4,
        out_specs=(anywhere,) * 4,
        scratch_shapes=[pltpu.SemaphoreType.DMA((4,))],
        name="store",
    )(*[pltpu.with_memory_space_constraint(a, pltpu.VMEM) for a in out])


def solution(mesh):
    placed = (
        P("seq", None),
        P(None, "head"),
        P(None, "head"),
        P("seq", "head"),
        P("seq", "head"),
        P("head", None, None),
    )

    def local(*args):
        out = shards(mesh.shape["seq"], *args)
        if mesh.shape["head"] == 1:
            return out
        return (lax.psum(out[0], "head"),) + tuple(out[1:])

    return jax.shard_map(
        local,
        mesh=mesh,
        in_specs=placed,
        out_specs=(P("seq", None), P("seq", "head"), P("seq", "head"), P("seq", "head")),
        check_vma=False,
    )
```

```python
import functools

import jax
import jax.numpy as jnp
from jax import lax
from jax.experimental import pallas as pl
from jax.experimental.pallas import tpu as pltpu
from jax.sharding import PartitionSpec as P

F32, BF16 = jnp.float32, jnp.bfloat16
LANES = 128
MESH = pl.DeviceIdType.MESH


def flipped(index, mask, stride=1):
    out, b = index, 0
    while mask >> b:
        if (mask >> b) & 1:
            bit = (index // (stride * 2**b)) % 2
            out = out + (1 - 2 * bit) * (stride * 2**b)
        b += 1
    return out


def radices(count):
    out = []
    while count > 1:
        out.append(4 if count % 4 == 0 else 2)
        count //= out[-1]
    return out


def dot(a, b):
    return jnp.dot(a, b, preferred_element_type=F32)


def dot_t(a, b):
    return lax.dot_general(a, b, (((1,), (1,)), ((), ())), preferred_element_type=F32)


def halves(x):
    high = x.astype(BF16)
    return high, (x - high.astype(F32)).astype(BF16)


def swap(x):
    return pltpu.roll(x, LANES // 2, 1)


def settle(ref, sem):
    pltpu.make_async_copy(ref, ref, sem).wait()


def remote(src, dst, send_sem, recv_sem, peer):
    return pltpu.make_async_remote_copy(
        src_ref=src, dst_ref=dst, send_sem=send_sem, recv_sem=recv_sem,
        device_id={"seq": peer}, device_id_type=MESH,
    )


def kernel(
    n, hid_h, wq_h, wk_h, val_h, gout_h, rf_h, o_hid, o_val, o_gq, o_gk,
    hid, wq, wk, val, gout, rf,
    hid_f, hid_r, kv_s, kv_a, qg_s, qg_a, rfs, rbs, feat_k, feat_q, bwd_x,
    ar_s, ar_r, pair_s, pair_r, dq_p, turned, feat_l, states, dq_a, gw_s, gw_r,
    in_ss, a2a_ss, a2a_rs, hid_ss, hid_rs, ar_ss, ar_rs, pair_ss, pair_rs, back_ss, back_rs,
    st_ss, st_rs, gw_ss, gw_rs,
):
    groups, head_dim, feats = rf.shape
    toks, width = hid.shape
    half = width // 2
    parts = half // LANES
    block = gw_s.shape[2]
    per = LANES // block
    pairs = groups // 2
    scale = head_dim ** (-0.25)
    norm = feats ** (-0.5)
    me = lax.axis_index("seq")
    mine = me % groups
    core = me % 2
    pair = mine // 2
    first = core == 0
    phases = radices(n // groups)
    partner = flipped(me, 1)

    barrier = pltpu.get_barrier_semaphore()

    def greet(step, carry):
        pl.semaphore_signal(
            barrier, inc=1, device_id={"seq": (me + step) % n}, device_id_type=MESH
        )
        return carry

    lax.fori_loop(1, n, greet, 0)
    loads = []
    for i, (src, dst) in enumerate(
        [(hid_h, hid), (wk_h, wk), (val_h, val), (wq_h, wq), (gout_h, gout), (rf_h, rf)]
    ):
        loads.append(pltpu.make_async_copy(src, dst, in_ss.at[i]))
        loads[-1].start()

    def low(shape):
        return lax.broadcasted_iota(jnp.int32, shape, 1) < head_dim

    def pack(proj, other, out):
        for p in range(pairs):
            a = proj[:, p * LANES : (p + 1) * LANES]
            b = other[:, p * LANES : (p + 1) * LANES].astype(F32)
            mask = low(a.shape)
            out[2 * p] = jnp.where(mask, a, swap(b))
            out[2 * p + 1] = jnp.where(mask, swap(a), b)

    def scatter(which, sent, got):
        for m in range(1, groups):
            to = flipped(me, m)
            remote(
                sent.at[to % groups], got.at[m], a2a_ss.at[which], a2a_rs.at[which, m // 2], to
            ).start()
        got[0] = sent[mine]

    def scattered(which, got, c):
        skip = 1 if c == 0 else 0
        settle(got.at[pl.ds(2 * c + skip, 2 - skip)], a2a_rs.at[which, c])

    for load in loads[:3]:
        load.wait()
    pack(dot(hid[...], wk[...]) * scale, val[...], kv_s)
    pl.semaphore_wait(barrier, n - 1)
    scatter(0, kv_s, kv_a)
    for load in loads[3:5]:
        load.wait()
    pack(dot(hid[...], wq[...]) * scale, gout[...], qg_s)
    scatter(1, qg_s, qg_a)

    for h in range(2):
        for q in range(parts):
            spot = h * half + q * LANES
            hid_f[h, q] = hid[:, spot : spot + LANES].astype(F32)

    relayed = [m for m in range(1, groups) if m & 6 == 6 and m < 8]
    direct = [m for m in range(1, groups) if m not in relayed]
    passed_on = [2, 5] if relayed else []
    ahead = 3

    def hidden_start(q, m):
        if m in relayed:
            via, hop = (2, 4) if m == 6 else (5, 2)
            source, to = hid_r.at[q, via], flipped(me, hop)
        else:
            to = flipped(me, m)
            source = hid_f.at[to % 2, q]
        recv = hid_rs.at[q, 1 if m in passed_on else 0]
        remote(source, hid_r.at[q, m], hid_ss.at[0], recv, to).start()

    def send_hidden(q):
        if q < parts:
            for m in passed_on + [m for m in direct if m not in passed_on]:
                hidden_start(q, m)
            hid_r[q, 0] = hid_f[core, q]

    for q in range(ahead):
        send_hidden(q)

    def relay(q):
        if q < parts:
            if passed_on:
                settle(hid_r.at[q, pl.ds(0, len(passed_on))], hid_rs.at[q, 1])
            for m in relayed:
                hidden_start(q, m)
            send_hidden(q + ahead)

    def hidden_rows(q):
        settle(hid_r.at[q, pl.ds(0, groups - 1 - len(passed_on))], hid_rs.at[q, 0])
        return hid_r[q].reshape(groups * toks, LANES).astype(BF16)

    loads[5].wait()
    for j in range(groups):
        rf_high, rf_low = halves(rf[j])
        rfs[j] = jnp.concatenate([rf_high, rf_high, rf_low, rf_low], axis=0)
        rbs[j] = jnp.concatenate([rf_high, rf_low], axis=0)

    def features(x, j):
        rows = jnp.where(low(x.shape), x, 0.0)
        high = rows.astype(BF16).astype(F32)
        both = (high + swap(rows - high)).astype(BF16)
        logits = dot(jnp.concatenate([both, both], axis=1), rfs[j])
        return jnp.exp(logits - 0.5 * jnp.sum(rows * rows, axis=1, keepdims=True)) * norm

    def chunk(ref, c):
        return ref[2 * c : 2 * c + 2].reshape(2 * toks, ref.shape[2])

    def all_reduce(which, total):
        stride = groups
        for f, radix in enumerate(phases):
            ar_s[which, f] = total
            for d in range(1, radix):
                remote(
                    ar_s.at[which, f], ar_r.at[which, f, d - 1],
                    ar_ss.at[which, f], ar_rs.at[which, f], flipped(me, d, stride),
                ).start()
            yield
            came = ar_r.at[which, f, pl.ds(0, radix - 1)]
            settle(came, ar_rs.at[which, f])
            settle(came, ar_ss.at[which, f])
            for d in range(radix - 1):
                total = total + ar_r[which, f, d]
            stride *= radix
        yield total

    def finish(steps):
        for got in steps:
            if got is not None:
                return got

    def spread(total):
        return halves(
            jnp.concatenate(
                [jnp.broadcast_to(total[7:8], (head_dim, feats)), total[8:]], axis=0
            )
        )

    lead = head_dim - 8

    for j in range(groups):
        feat_l[j] = features(kv_s[j], j)

    total = jnp.zeros((LANES, feats), F32)
    for c in range(pairs):
        scattered(0, kv_a, c)
        x = chunk(kv_a, c)
        b = features(x, mine)
        feat_k[c] = b
        high, rest = halves(b)
        ones = jnp.where(low(x.shape), 1.0, x).T.astype(BF16)
        total = total + dot(ones, high) + dot(ones, rest)
    reduce_k = all_reduce(0, total[lead:])
    next(reduce_k)

    for c in range(pairs):
        scattered(1, qg_a, c)
        feat_q[c] = features(chunk(qg_a, c), mine)

    st_high, st_low = spread(finish(reduce_k))
    st_both = jnp.concatenate([st_high, st_low], axis=0)
    total = jnp.zeros((LANES, feats), F32)
    for c in range(pairs):
        x = chunk(qg_a, c)
        high, rest = halves(feat_q[c])
        nd = dot_t(high, st_both)
        nd = nd[:, :LANES] + nd[:, LANES:] + dot_t(rest, st_high)
        mask = low(nd.shape)
        den = jnp.where(mask, nd, swap(nd))
        upstream = jnp.where(mask, 0.0, x) / den
        grad_den = -jnp.sum(upstream * nd / den, axis=1, keepdims=True)
        lane = lax.broadcasted_iota(jnp.int32, nd.shape, 1)
        xg = jnp.where(lane == head_dim - 1, grad_den, upstream)
        bwd_x[c] = xg
        turned_high, turned_low = halves(xg.T)
        total = total + dot(turned_high, high) + dot(turned_low, high) + dot(turned_high, rest)
    reduce_q = all_reduce(1, total[lead:])
    next(reduce_q)
    relay(0)

    def feature_grad(x, weighted, j):
        high, rest = halves(weighted)
        back = dot_t(high, rbs[j]) + dot_t(rest, rbs[j])
        back = back + swap(back)
        out = (back - x * jnp.sum(weighted, axis=1, keepdims=True)) * scale
        return jnp.where(low(x.shape), out.astype(BF16).astype(F32), 0.0)

    def pair_send(which, c, out):
        placed = jnp.where(first, out, swap(out))
        pair_s[which, 2 * c] = placed[:toks]
        pair_s[which, 2 * c + 1] = placed[toks:]
        two = pl.ds(2 * c, 2)
        remote(
            pair_s.at[which, two], pair_r.at[which, two],
            pair_ss.at[which], pair_rs.at[which, c], partner,
        ).start()

    def paired(which, c):
        settle(pair_r.at[which, pl.ds(2 * c, 2)], pair_rs.at[which, c])
        for m in (2 * c, 2 * c + 1):
            both = pair_s[which, m] + pair_r[which, m ^ 1]
            turned[which, :, m * toks : (m + 1) * toks] = both.T.astype(BF16)
            if which == 0:
                dq_p[m] = both

    for c in range(pairs):
        x = chunk(qg_a, c)
        high, rest = halves(bwd_x[c])
        grads = dot(
            jnp.concatenate([high, rest], axis=1), jnp.concatenate([st_high, st_high], axis=0)
        ) + dot(high, st_low)
        pair_send(0, c, feature_grad(x, feat_q[c] * grads, mine))

    relay(1)
    for c in range(pairs):
        paired(0, c)

    def weight_part(which, q, rows):
        total = dot(turned[which], rows).T
        gw_s[which, q * per : (q + 1) * per] = total.reshape(per, block, LANES)

    def weight_sends(which, q):
        def start(i, carry):
            to = core * (n // 2) + i

            @pl.when(to != me)
            def _():
                remote(
                    gw_s.at[which, i], gw_r.at[which, me // 2],
                    gw_ss.at[which], gw_rs.at[which], to,
                ).start()

            @pl.when(to == me)
            def _():
                pltpu.make_async_copy(
                    gw_s.at[which, i], gw_r.at[which, me // 2], gw_rs.at[which]
                ).start()

            return carry

        lax.fori_loop(q * per, (q + 1) * per, start, 0)

    relay(2)
    weight_part(0, 0, hidden_rows(0))

    total = finish(reduce_q)
    states[mine] = total

    def state_send(to, slot, which):
        remote(states.at[slot], states.at[slot], st_ss.at[0], st_rs.at[which], to).start()

    weight_sends(0, 0)

    def value_rows(x):
        lane = lax.broadcasted_iota(jnp.int32, x.shape, 1)
        ones = jnp.where(lane == head_dim - 1, 1.0, 0.0)
        xv = jnp.where(low(x.shape), ones, x).astype(BF16)
        return jnp.concatenate([xv, xv], axis=1)

    gs_high, gs_low = spread(total)
    gs_both = jnp.concatenate([gs_high, gs_low], axis=0)
    for c in range(pairs):
        x = chunk(kv_a, c)
        grads = dot(value_rows(x), gs_both)
        pair_send(1, c, feature_grad(x, feat_k[c] * grads, mine))
        if c == pairs // 2 - 1:
            relay(3)
    for m in range(2, groups, 2):
        state_send(flipped(me, m), mine, 0)
    state_send(partner, mine, 1)
    weight_part(0, 1, hidden_rows(1))
    weight_sends(0, 1)
    for c in range(pairs):
        paired(1, c)
    for m in range(2, groups, 2):
        remote(
            dq_p.at[m], dq_a.at[pair], back_ss.at[0], back_rs.at[0], flipped(me, m)
        ).start()
    dq_a[pair] = dq_p[0]
    for q in range(2):
        weight_part(1, q, hid_r[q].reshape(groups * toks, LANES).astype(BF16))
        weight_sends(1, q)
    for q in range(2, parts):
        if q > 2:
            relay(q + 1)
        rows = hidden_rows(q)
        for which in range(2):
            weight_part(which, q, rows)
            weight_sends(which, q)

    if pairs > 1:
        settle(states.at[pl.ds(0, pairs - 1)], st_rs.at[0])
    for m in range(2, groups, 2):
        state_send(partner, flipped(me, m) % groups, 1)
    settle(states.at[pl.ds(0, pairs)], st_rs.at[1])
    dk_slabs = []
    for p in range(pairs):
        outs = []
        for j in (2 * p, 2 * p + 1):
            gs_high, gs_low = spread(states[j])
            gs_both = jnp.concatenate([gs_high, gs_low], axis=0)
            x, b = kv_s[j], feat_l[j]
            out = feature_grad(x, b * dot(value_rows(x), gs_both), j)
            high, rest = halves(b)
            gv = dot_t(high, gs_both)
            gv = gv[:, :LANES] + gv[:, LANES:] + dot_t(rest, gs_high)
            outs.append((out, gv))
        (dk_one, gv_one), (dk_two, gv_two) = outs
        mask = low(dk_one.shape)
        dk_slabs.append(jnp.where(mask, dk_one, swap(dk_two)))
        slab = jnp.where(mask, swap(gv_one), gv_two)
        o_val[:, p * LANES : (p + 1) * LANES] = slab.astype(BF16)
    o_hid[...] = dot_t(jnp.concatenate(dk_slabs, axis=1).astype(BF16), wk[...])
    settle(dq_a.at[pl.ds(0, pairs - 1)], back_rs.at[0])
    dq_all = jnp.concatenate([dq_a[p] for p in range(pairs)], axis=1).astype(BF16)
    o_hid[...] += dot_t(dq_all, wq[...])

    for which in range(2):
        settle(gw_r.at[which], gw_rs.at[which])
    for which, out in ((0, o_gq), (1, o_gk)):
        for p in range(pairs):
            total = gw_r[which, p]
            for i in range(p + pairs, n // 2, pairs):
                total = total + gw_r[which, i]
            out[:, p * LANES : (p + 1) * LANES] = total
    for which in range(2):
        others = kv_a.at[pl.ds(1, groups - 1)]
        settle(others, a2a_ss.at[which])
        settle(pair_s.at[which], pair_ss.at[which])
        own_set = me // (n // 2) == core

        @pl.when(own_set)
        def _():
            settle(gw_s.at[which, pl.ds(0, n // 2 - 1)], gw_ss.at[which])

        @pl.when(jnp.logical_not(own_set))
        def _():
            settle(gw_s.at[which], gw_ss.at[which])

    settle(dq_a.at[pl.ds(0, pairs - 1)], back_ss.at[0])
    settle(states.at[pl.ds(0, groups - 1)], st_ss.at[0])
    settle(hid_r.at[:, pl.ds(1, groups - 1)], hid_ss.at[0])


def store(*refs):
    count = len(refs) // 2
    sems = refs[-1]
    copies = [
        pltpu.make_async_copy(refs[i], refs[count + i], sems.at[i]) for i in range(count)
    ]
    for copy in copies:
        copy.start()
    for copy in copies:
        copy.wait()


def shards(n, *args):
    hidden, random_feats = args[0], args[5]
    toks, width = hidden.shape
    groups, head_dim, feats = random_feats.shape
    cols = groups * head_dim
    pairs = groups // 2
    block = width // n
    parts = width // 2 // LANES
    phases = len(radices(n // groups))
    rows = head_dim + 8
    tok_block = (groups, toks, LANES)
    scratch = [pltpu.VMEM(a.shape, a.dtype) for a in args]
    scratch += [
        pltpu.VMEM((2, parts, toks, LANES), F32),
        pltpu.VMEM((parts,) + tok_block, F32),
    ]
    scratch += [pltpu.VMEM(tok_block, F32)] * 4
    scratch += [
        pltpu.VMEM((groups, 4 * head_dim, feats), BF16),
        pltpu.VMEM((groups, 2 * head_dim, feats), BF16),
        pltpu.VMEM((pairs, 2 * toks, feats), F32),
        pltpu.VMEM((pairs, 2 * toks, feats), F32),
        pltpu.VMEM((pairs, 2 * toks, LANES), F32),
        pltpu.VMEM((2, phases, rows, feats), F32),
        pltpu.VMEM((2, phases, 3, rows, feats), F32),
    ]
    scratch += [pltpu.VMEM((2,) + tok_block, F32)] * 2
    scratch += [
        pltpu.VMEM(tok_block, F32),
        pltpu.VMEM((2, LANES, groups * toks), BF16),
        pltpu.VMEM((groups, toks, feats), F32),
        pltpu.VMEM((groups, rows, feats), F32),
        pltpu.VMEM((pairs, toks, LANES), F32),
    ]
    scratch += [pltpu.VMEM((2, n // 2, block, LANES), F32)] * 2
    for shape in (
        (6,), (2,), (2, pairs), (1,), (parts, 2), (2, phases), (2, phases), (2,), (2, pairs),
        (1,), (1,), (1,), (2,), (2,), (2,),
    ):
        scratch.append(pltpu.SemaphoreType.DMA(shape))
    vmem = pl.BlockSpec(memory_space=pltpu.VMEM)
    anywhere = pl.BlockSpec(memory_space=pl.ANY)
    shapes = (
        jax.ShapeDtypeStruct((toks, width), F32),
        jax.ShapeDtypeStruct((toks, cols), BF16),
        jax.ShapeDtypeStruct((block, cols), F32),
        jax.ShapeDtypeStruct((block, cols), F32),
    )
    out = pl.pallas_call(
        functools.partial(kernel, n),
        out_shape=tuple(pltpu.VMEM(a.shape, a.dtype) for a in shapes),
        in_specs=[anywhere] * 6,
        out_specs=(vmem,) * 4,
        scratch_shapes=scratch,
        compiler_params=pltpu.CompilerParams(
            collective_id=0, has_side_effects=True, vmem_limit_bytes=56 * 2**20
        ),
        name="backward",
    )(*args)
    return pl.pallas_call(
        store,
        out_shape=shapes,
        in_specs=[vmem] * 4,
        out_specs=(anywhere,) * 4,
        scratch_shapes=[pltpu.SemaphoreType.DMA((4,))],
        name="store",
    )(*[pltpu.with_memory_space_constraint(a, pltpu.VMEM) for a in out])


def solution(mesh):
    placed = (
        P("seq", None),
        P(None, "head"),
        P(None, "head"),
        P("seq", "head"),
        P("seq", "head"),
        P("head", None, None),
    )

    def local(*args):
        out = shards(mesh.shape["seq"], *args)
        if mesh.shape["head"] == 1:
            return out
        return (lax.psum(out[0], "head"),) + tuple(out[1:])

    return jax.shard_map(
        local,
        mesh=mesh,
        in_specs=placed,
        out_specs=(P("seq", None), P("seq", "head"), P("seq", "head"), P("seq", "head")),
        check_vma=False,
    )
```

```python
import functools

import jax
import jax.numpy as jnp
from jax import lax
from jax.experimental import pallas as pl
from jax.experimental.pallas import tpu as pltpu
from jax.sharding import PartitionSpec as P

F32, BF16 = jnp.float32, jnp.bfloat16
LANES = 128
MESH = pl.DeviceIdType.MESH


def flipped(index, mask, stride=1):
    out, b = index, 0
    while mask >> b:
        if (mask >> b) & 1:
            bit = (index // (stride * 2**b)) % 2
            out = out + (1 - 2 * bit) * (stride * 2**b)
        b += 1
    return out


def radices(count):
    out = []
    while count > 1:
        out.append(4 if count % 4 == 0 else 2)
        count //= out[-1]
    return out


def dot(a, b):
    return jnp.dot(a, b, preferred_element_type=F32)


def dot_t(a, b):
    return lax.dot_general(a, b, (((1,), (1,)), ((), ())), preferred_element_type=F32)


def halves(x):
    high = x.astype(BF16)
    return high, (x - high.astype(F32)).astype(BF16)


def swap(x):
    return pltpu.roll(x, LANES // 2, 1)


def settle(ref, sem):
    pltpu.make_async_copy(ref, ref, sem).wait()


def remote(src, dst, send_sem, recv_sem, peer):
    return pltpu.make_async_remote_copy(
        src_ref=src, dst_ref=dst, send_sem=send_sem, recv_sem=recv_sem,
        device_id={"seq": peer}, device_id_type=MESH,
    )


def kernel(
    n, hid_h, wq_h, wk_h, val_h, gout_h, rf_h, o_hid, o_val, o_gq, o_gk,
    hid, wq, wk, val, gout, rf,
    hid_f, hid_r, kv_s, kv_a, qg_s, qg_a, rfs, rbs, feat_k, feat_q, bwd_x,
    ar_s, ar_r, pair_s, pair_r, dq_p, turned, feat_l, states, dq_a, gw_s, gw_x, gw_r,
    in_ss, a2a_ss, a2a_rs, hid_ss, hid_rs, ar_ss, ar_rs, pair_ss, pair_rs, back_ss, back_rs,
    st_ss, st_rs, gw_ss, gw_xs, gw_rs,
):
    groups, head_dim, feats = rf.shape
    toks, width = hid.shape
    half = width // 2
    parts = half // LANES
    block = gw_s.shape[3]
    per = LANES // block
    later = parts // 2
    pairs = groups // 2
    scale = head_dim ** (-0.25)
    norm = feats ** (-0.5)
    me = lax.axis_index("seq")
    mine = me % groups
    core = me % 2
    pair = mine // 2
    first = core == 0
    phases = radices(n // groups)
    partner = flipped(me, 1)
    parity = (me // groups) % 2
    plane_next = flipped(me, 1, groups)
    order = [(i + (1 - parity) * later) % parts for i in range(parts)]

    barrier = pltpu.get_barrier_semaphore()

    def greet(step, carry):
        pl.semaphore_signal(
            barrier, inc=1, device_id={"seq": (me + step) % n}, device_id_type=MESH
        )
        return carry

    loads = []
    for i, (src, dst) in enumerate(
        [(hid_h, hid), (wk_h, wk), (val_h, val), (wq_h, wq), (gout_h, gout), (rf_h, rf)]
    ):
        loads.append(pltpu.make_async_copy(src, dst, in_ss.at[i]))
    for load in loads[:3]:
        load.start()
    lax.fori_loop(1, n, greet, 0)

    def low(shape):
        return lax.broadcasted_iota(jnp.int32, shape, 1) < head_dim

    def pack(proj, other, out):
        for p in range(pairs):
            a = proj[:, p * LANES : (p + 1) * LANES]
            b = other[:, p * LANES : (p + 1) * LANES].astype(F32)
            mask = low(a.shape)
            out[2 * p] = jnp.where(mask, a, swap(b))
            out[2 * p + 1] = jnp.where(mask, swap(a), b)

    def scatter(which, sent, got):
        for m in range(1, groups):
            to = flipped(me, m)
            remote(
                sent.at[to % groups], got.at[m], a2a_ss.at[which], a2a_rs.at[which, m // 2], to
            ).start()
        got[0] = sent[mine]

    def scattered(which, got, c):
        skip = 1 if c == 0 else 0
        settle(got.at[pl.ds(2 * c + skip, 2 - skip)], a2a_rs.at[which, c])

    for load in loads[:3]:
        load.wait()
    for load in loads[3:]:
        load.start()
    pack(dot(hid[...], wk[...]) * scale, val[...], kv_s)
    pl.semaphore_wait(barrier, n - 1)
    scatter(0, kv_s, kv_a)
    for load in loads[3:5]:
        load.wait()
    pack(dot(hid[...], wq[...]) * scale, gout[...], qg_s)
    scatter(1, qg_s, qg_a)

    for h in range(2):
        for q in range(parts):
            spot = pl.multiple_of(h * half + order[q] * LANES, LANES)
            hid_f[h, q] = hid[:, pl.ds(spot, LANES)].astype(F32)

    relayed = [m for m in range(1, groups) if m & 6 == 6 and m < 8]
    direct = [m for m in range(1, groups) if m not in relayed]
    passed_on = [2, 5] if relayed else []
    ahead = 3

    def hidden_start(q, m):
        if m in relayed:
            via, hop = (2, 4) if m == 6 else (5, 2)
            source, to = hid_r.at[q, via], flipped(me, hop)
        else:
            to = flipped(me, m)
            source = hid_f.at[to % 2, q]
        recv = hid_rs.at[q, 1 if m in passed_on else 0]
        remote(source, hid_r.at[q, m], hid_ss.at[0], recv, to).start()

    def send_hidden(q):
        if q < parts:
            for m in passed_on + [m for m in direct if m not in passed_on]:
                hidden_start(q, m)
            hid_r[q, 0] = hid_f[core, q]

    for q in range(ahead):
        send_hidden(q)

    def relay(q):
        if q < parts:
            if passed_on:
                settle(hid_r.at[q, pl.ds(0, len(passed_on))], hid_rs.at[q, 1])
            for m in relayed:
                hidden_start(q, m)
            send_hidden(q + ahead)

    def hidden_rows(q):
        settle(hid_r.at[q, pl.ds(0, groups - 1 - len(passed_on))], hid_rs.at[q, 0])
        return hid_r[q].reshape(groups * toks, LANES).astype(BF16)

    loads[5].wait()
    for j in range(groups):
        rf_high, rf_low = halves(rf[j])
        rfs[j] = jnp.concatenate([rf_high, rf_high, rf_low, rf_low], axis=0)
        rbs[j] = jnp.concatenate([rf_high, rf_low], axis=0)

    def features(x, j):
        rows = jnp.where(low(x.shape), x, 0.0)
        high = rows.astype(BF16).astype(F32)
        both = (high + swap(rows - high)).astype(BF16)
        logits = dot(jnp.concatenate([both, both], axis=1), rfs[j])
        return jnp.exp(logits - 0.5 * jnp.sum(rows * rows, axis=1, keepdims=True)) * norm

    def chunk(ref, c):
        return ref[2 * c : 2 * c + 2].reshape(2 * toks, ref.shape[2])

    def all_reduce(which, total):
        stride = groups
        for f, radix in enumerate(phases):
            ar_s[which, f] = total
            for d in range(1, radix):
                remote(
                    ar_s.at[which, f], ar_r.at[which, f, d - 1],
                    ar_ss.at[which, f], ar_rs.at[which, f], flipped(me, d, stride),
                ).start()
            yield
            came = ar_r.at[which, f, pl.ds(0, radix - 1)]
            settle(came, ar_rs.at[which, f])
            settle(came, ar_ss.at[which, f])
            for d in range(radix - 1):
                total = total + ar_r[which, f, d]
            stride *= radix
        yield total

    def finish(steps):
        for got in steps:
            if got is not None:
                return got

    def spread(total):
        return halves(
            jnp.concatenate(
                [jnp.broadcast_to(total[7:8], (head_dim, feats)), total[8:]], axis=0
            )
        )

    lead = head_dim - 8

    for j in range(groups):
        feat_l[j] = features(kv_s[j], j)

    total = jnp.zeros((LANES, feats), F32)
    for c in range(pairs):
        scattered(0, kv_a, c)
        x = chunk(kv_a, c)
        b = features(x, mine)
        feat_k[c] = b
        high, rest = halves(b)
        ones = jnp.where(low(x.shape), 1.0, x).T.astype(BF16)
        total = total + dot(ones, high) + dot(ones, rest)
    reduce_k = all_reduce(0, total[lead:])
    next(reduce_k)

    for c in range(pairs):
        scattered(1, qg_a, c)
        feat_q[c] = features(chunk(qg_a, c), mine)

    st_high, st_low = spread(finish(reduce_k))
    st_both = jnp.concatenate([st_high, st_low], axis=0)
    total = jnp.zeros((LANES, feats), F32)
    for c in range(pairs):
        x = chunk(qg_a, c)
        high, rest = halves(feat_q[c])
        nd = dot_t(high, st_both)
        nd = nd[:, :LANES] + nd[:, LANES:] + dot_t(rest, st_high)
        mask = low(nd.shape)
        den = jnp.where(mask, nd, swap(nd))
        upstream = jnp.where(mask, 0.0, x) / den
        grad_den = -jnp.sum(upstream * nd / den, axis=1, keepdims=True)
        lane = lax.broadcasted_iota(jnp.int32, nd.shape, 1)
        xg = jnp.where(lane == head_dim - 1, grad_den, upstream)
        bwd_x[c] = xg
        turned_high, turned_low = halves(xg.T)
        total = total + dot(turned_high, high) + dot(turned_low, high) + dot(turned_high, rest)
    reduce_q = all_reduce(1, total[lead:])
    next(reduce_q)
    relay(0)

    def feature_grad(x, weighted, j):
        high, rest = halves(weighted)
        back = dot_t(high, rbs[j]) + dot_t(rest, rbs[j])
        back = back + swap(back)
        out = (back - x * jnp.sum(weighted, axis=1, keepdims=True)) * scale
        return jnp.where(low(x.shape), out.astype(BF16).astype(F32), 0.0)

    def pair_send(which, outs):
        for c, out in outs:
            pair_s[which, c] = out[:toks] + swap(out[toks:])
        for c, _ in outs:
            remote(
                pair_s.at[which, c], pair_r.at[which, c],
                pair_ss.at[which], pair_rs.at[which, c], partner,
            ).start()

    def paired(which, c):
        settle(pair_r.at[which, c], pair_rs.at[which, c])
        own, theirs = pair_s[which, c], pair_r[which, c]
        mask = low(own.shape)
        for m, a, b in ((2 * c, own, swap(theirs)), (2 * c + 1, swap(own), theirs)):
            both = jnp.where(first, jnp.where(mask, a, swap(b)), jnp.where(mask, b, swap(a)))
            turned[which, :, m * toks : (m + 1) * toks] = both.T.astype(BF16)
            if which == 0:
                dq_p[m] = both

    def query_grad(c):
        x = chunk(qg_a, c)
        high, rest = halves(bwd_x[c])
        grads = dot(
            jnp.concatenate([high, rest], axis=1), jnp.concatenate([st_high, st_high], axis=0)
        ) + dot(high, st_low)
        return c, feature_grad(x, feat_q[c] * grads, mine)

    for c in range(0, pairs, 2):
        pair_send(0, [query_grad(c), query_grad(c + 1)])

    relay(1)
    for c in range(pairs):
        paired(0, c)

    def weight_part(which, q, rows):
        total = dot(turned[which], rows).T.reshape(per, block, LANES)
        if q < later:
            gw_s[which, q] = total
            remote(
                gw_s.at[which, q], gw_x.at[which, q], gw_ss.at[2], gw_xs.at[which, q], plane_next
            ).start()
            return
        settle(gw_x.at[which, q - later], gw_xs.at[which, q - later])
        gw_s[which, q] = total + gw_x[which, q - later]
        slot = (me // groups) // 2 * pairs + pair

        def start(i, carry):
            to = core * (n // 2) + order[q] * per + i

            @pl.when(to != me)
            def _():
                remote(
                    gw_s.at[which, q, i], gw_r.at[which, slot], gw_ss.at[which], gw_rs.at[which], to
                ).start()

            @pl.when(to == me)
            def _():
                pltpu.make_async_copy(
                    gw_s.at[which, q, i], gw_r.at[which, slot], gw_rs.at[which]
                ).start()

            return carry

        lax.fori_loop(0, per, start, 0)

    relay(2)
    weight_part(0, 0, hidden_rows(0))

    total = finish(reduce_q)
    states[mine] = total

    def state_send(to, slot, which):
        remote(states.at[slot], states.at[slot], st_ss.at[0], st_rs.at[which], to).start()


    def value_rows(x):
        lane = lax.broadcasted_iota(jnp.int32, x.shape, 1)
        ones = jnp.where(lane == head_dim - 1, 1.0, 0.0)
        xv = jnp.where(low(x.shape), ones, x).astype(BF16)
        return jnp.concatenate([xv, xv], axis=1)

    gs_high, gs_low = spread(total)
    gs_both = jnp.concatenate([gs_high, gs_low], axis=0)

    def key_grad(c):
        x = chunk(kv_a, c)
        return c, feature_grad(x, feat_k[c] * dot(value_rows(x), gs_both), mine)

    for c in range(0, pairs, 2):
        pair_send(1, [key_grad(c), key_grad(c + 1)])
        if c == 0:
            relay(3)
    for m in range(2, groups, 2):
        state_send(flipped(me, m), mine, 0)
    state_send(partner, mine, 1)
    weight_part(0, 1, hidden_rows(1))
    for c in range(pairs):
        paired(1, c)
    for m in range(2, groups, 2):
        remote(
            dq_p.at[m], dq_a.at[pair], back_ss.at[0], back_rs.at[0], flipped(me, m)
        ).start()
    dq_a[pair] = dq_p[0]
    for q in range(2):
        weight_part(1, q, hid_r[q].reshape(groups * toks, LANES).astype(BF16))
    for q in range(2, parts):
        if q > 2:
            relay(q + 1)
        rows = hidden_rows(q)
        for which in range(2):
            weight_part(which, q, rows)

    if pairs > 1:
        settle(states.at[pl.ds(0, pairs - 1)], st_rs.at[0])
    for m in range(2, groups, 2):
        state_send(partner, flipped(me, m) % groups, 1)
    settle(states.at[pl.ds(0, pairs)], st_rs.at[1])
    dk_slabs = []
    for p in range(pairs):
        outs = []
        for j in (2 * p, 2 * p + 1):
            gs_high, gs_low = spread(states[j])
            gs_both = jnp.concatenate([gs_high, gs_low], axis=0)
            x, b = kv_s[j], feat_l[j]
            out = feature_grad(x, b * dot(value_rows(x), gs_both), j)
            high, rest = halves(b)
            gv = dot_t(high, gs_both)
            gv = gv[:, :LANES] + gv[:, LANES:] + dot_t(rest, gs_high)
            outs.append((out, gv))
        (dk_one, gv_one), (dk_two, gv_two) = outs
        mask = low(dk_one.shape)
        dk_slabs.append(jnp.where(mask, dk_one, swap(dk_two)))
        slab = jnp.where(mask, swap(gv_one), gv_two)
        o_val[:, p * LANES : (p + 1) * LANES] = slab.astype(BF16)
    o_hid[...] = dot_t(jnp.concatenate(dk_slabs, axis=1).astype(BF16), wk[...])
    settle(dq_a.at[pl.ds(0, pairs - 1)], back_rs.at[0])
    dq_all = jnp.concatenate([dq_a[p] for p in range(pairs)], axis=1).astype(BF16)
    o_hid[...] += dot_t(dq_all, wq[...])

    for which in range(2):
        settle(gw_r.at[which], gw_rs.at[which])
    for which, out in ((0, o_gq), (1, o_gk)):
        for p in range(pairs):
            total = gw_r[which, p]
            for i in range(p + pairs, n // 4, pairs):
                total = total + gw_r[which, i]
            out[:, p * LANES : (p + 1) * LANES] = total
    for which in range(2):
        others = kv_a.at[pl.ds(1, groups - 1)]
        settle(others, a2a_ss.at[which])
        settle(pair_s.at[which], pair_ss.at[which])
        own_set = me // (n // 4) == 2 * core + parity

        @pl.when(own_set)
        def _():
            settle(gw_r.at[which, pl.ds(0, n // 4 - 1)], gw_ss.at[which])

        @pl.when(jnp.logical_not(own_set))
        def _():
            settle(gw_r.at[which], gw_ss.at[which])

    settle(gw_x, gw_ss.at[2])
    settle(dq_a.at[pl.ds(0, pairs - 1)], back_ss.at[0])
    settle(states.at[pl.ds(0, groups - 1)], st_ss.at[0])
    settle(hid_r.at[:, pl.ds(1, groups - 1)], hid_ss.at[0])


def store(*refs):
    count = len(refs) // 2
    sems = refs[-1]
    copies = [
        pltpu.make_async_copy(refs[i], refs[count + i], sems.at[i]) for i in range(count)
    ]
    for copy in copies:
        copy.start()
    for copy in copies:
        copy.wait()


def shards(n, *args):
    hidden, random_feats = args[0], args[5]
    toks, width = hidden.shape
    groups, head_dim, feats = random_feats.shape
    cols = groups * head_dim
    pairs = groups // 2
    block = width // n
    parts = width // 2 // LANES
    phases = len(radices(n // groups))
    rows = head_dim + 8
    tok_block = (groups, toks, LANES)
    scratch = [pltpu.VMEM(a.shape, a.dtype) for a in args]
    scratch += [
        pltpu.VMEM((2, parts, toks, LANES), F32),
        pltpu.VMEM((parts,) + tok_block, F32),
    ]
    scratch += [pltpu.VMEM(tok_block, F32)] * 4
    scratch += [
        pltpu.VMEM((groups, 4 * head_dim, feats), BF16),
        pltpu.VMEM((groups, 2 * head_dim, feats), BF16),
        pltpu.VMEM((pairs, 2 * toks, feats), F32),
        pltpu.VMEM((pairs, 2 * toks, feats), F32),
        pltpu.VMEM((pairs, 2 * toks, LANES), F32),
        pltpu.VMEM((2, phases, rows, feats), F32),
        pltpu.VMEM((2, phases, 3, rows, feats), F32),
    ]
    scratch += [pltpu.VMEM((2, pairs, toks, LANES), F32)] * 2
    scratch += [
        pltpu.VMEM(tok_block, F32),
        pltpu.VMEM((2, LANES, groups * toks), BF16),
        pltpu.VMEM((groups, toks, feats), F32),
        pltpu.VMEM((groups, rows, feats), F32),
        pltpu.VMEM((pairs, toks, LANES), F32),
    ]
    scratch += [
        pltpu.VMEM((2, parts, LANES // block, block, LANES), F32),
        pltpu.VMEM((2, parts // 2, LANES // block, block, LANES), F32),
        pltpu.VMEM((2, n // 4, block, LANES), F32),
    ]
    for shape in (
        (6,), (2,), (2, pairs), (1,), (parts, 2), (2, phases), (2, phases), (2,), (2, pairs),
        (1,), (1,), (1,), (2,), (3,), (2, parts // 2), (2,),
    ):
        scratch.append(pltpu.SemaphoreType.DMA(shape))
    vmem = pl.BlockSpec(memory_space=pltpu.VMEM)
    anywhere = pl.BlockSpec(memory_space=pl.ANY)
    shapes = (
        jax.ShapeDtypeStruct((toks, width), F32),
        jax.ShapeDtypeStruct((toks, cols), BF16),
        jax.ShapeDtypeStruct((block, cols), F32),
        jax.ShapeDtypeStruct((block, cols), F32),
    )
    out = pl.pallas_call(
        functools.partial(kernel, n),
        out_shape=tuple(pltpu.VMEM(a.shape, a.dtype) for a in shapes),
        in_specs=[anywhere] * 6,
        out_specs=(vmem,) * 4,
        scratch_shapes=scratch,
        compiler_params=pltpu.CompilerParams(
            collective_id=0, has_side_effects=True, vmem_limit_bytes=56 * 2**20
        ),
        name="backward",
    )(*args)
    return pl.pallas_call(
        store,
        out_shape=shapes,
        in_specs=[vmem] * 4,
        out_specs=(anywhere,) * 4,
        scratch_shapes=[pltpu.SemaphoreType.DMA((4,))],
        name="store",
    )(*[pltpu.with_memory_space_constraint(a, pltpu.VMEM) for a in out])


def solution(mesh):
    placed = (
        P("seq", None),
        P(None, "head"),
        P(None, "head"),
        P("seq", "head"),
        P("seq", "head"),
        P("head", None, None),
    )

    def local(*args):
        out = shards(mesh.shape["seq"], *args)
        if mesh.shape["head"] == 1:
            return out
        return (lax.psum(out[0], "head"),) + tuple(out[1:])

    return jax.shard_map(
        local,
        mesh=mesh,
        in_specs=placed,
        out_specs=(P("seq", None), P("seq", "head"), P("seq", "head"), P("seq", "head")),
        check_vma=False,
    )
```

```python
import functools

import jax
import jax.numpy as jnp
from jax import lax
from jax.experimental import pallas as pl
from jax.experimental.pallas import tpu as pltpu
from jax.sharding import PartitionSpec as P

F32, BF16 = jnp.float32, jnp.bfloat16
LANES = 128
MESH = pl.DeviceIdType.MESH


def flipped(index, mask, stride=1):
    out, b = index, 0
    while mask >> b:
        if (mask >> b) & 1:
            bit = (index // (stride * 2**b)) % 2
            out = out + (1 - 2 * bit) * (stride * 2**b)
        b += 1
    return out


def radices(count):
    out = []
    while count > 1:
        out.append(4 if count % 4 == 0 else 2)
        count //= out[-1]
    return out


def dot(a, b):
    return jnp.dot(a, b, preferred_element_type=F32)


def dot_t(a, b):
    return lax.dot_general(a, b, (((1,), (1,)), ((), ())), preferred_element_type=F32)


def halves(x):
    high = x.astype(BF16)
    return high, (x - high.astype(F32)).astype(BF16)


def swap(x):
    return pltpu.roll(x, LANES // 2, 1)


def settle(ref, sem):
    pltpu.make_async_copy(ref, ref, sem).wait()


def remote(src, dst, send_sem, recv_sem, peer):
    return pltpu.make_async_remote_copy(
        src_ref=src, dst_ref=dst, send_sem=send_sem, recv_sem=recv_sem,
        device_id={"seq": peer}, device_id_type=MESH,
    )


def kernel(
    n, hid_h, wq_h, wk_h, val_h, gout_h, rf_h, o_hid, o_val, o_gq, o_gk,
    hid, wq, wk, val, gout, rf,
    hid_f, hid_r, kv_s, kv_a, qg_s, qg_a, rfs, rbs, feat_k, feat_q, feat_h, bwd_x,
    ar_s, ar_r, pair_s, pair_r, dq_p, turned, feat_l, states, dq_a, gw_s, gw_x, gw_r,
    in_ss, a2a_ss, a2a_rs, hid_ss, hid_rs, ar_ss, ar_rs, pair_ss, pair_rs, back_ss, back_rs,
    st_ss, st_rs, gw_ss, gw_xs, gw_rs,
):
    groups, head_dim, feats = rf.shape
    toks, width = hid.shape
    half = width // 2
    parts = half // LANES
    block = gw_s.shape[3]
    per = LANES // block
    later = parts // 2
    pairs = groups // 2
    scale = head_dim ** (-0.25)
    norm = feats ** (-0.5)
    me = lax.axis_index("seq")
    mine = me % groups
    core = me % 2
    pair = mine // 2
    first = core == 0
    phases = radices(n // groups)
    partner = flipped(me, 1)
    parity = (me // groups) % 2
    plane_next = flipped(me, 1, groups)
    order = [(i + (1 - parity) * later) % parts for i in range(parts)]

    barrier = pltpu.get_barrier_semaphore()

    def greet(step, carry):
        pl.semaphore_signal(
            barrier, inc=1, device_id={"seq": (me + step) % n}, device_id_type=MESH
        )
        return carry

    loads = []
    for i, (src, dst) in enumerate(
        [(hid_h, hid), (wk_h, wk), (val_h, val), (wq_h, wq), (gout_h, gout), (rf_h, rf)]
    ):
        loads.append(pltpu.make_async_copy(src, dst, in_ss.at[i]))
    for load in loads[:3]:
        load.start()
    lax.fori_loop(1, n, greet, 0)

    def low(shape):
        return lax.broadcasted_iota(jnp.int32, shape, 1) < head_dim

    def pack(proj, other, out):
        for p in range(pairs):
            a = proj[:, p * LANES : (p + 1) * LANES]
            b = other[:, p * LANES : (p + 1) * LANES].astype(F32)
            mask = low(a.shape)
            out[2 * p] = jnp.where(mask, a, swap(b))
            out[2 * p + 1] = jnp.where(mask, swap(a), b)

    def scatter(which, sent, got):
        for m in range(1, groups):
            to = flipped(me, m)
            remote(
                sent.at[to % groups], got.at[m], a2a_ss.at[which], a2a_rs.at[which, m // 2], to
            ).start()
        got[0] = sent[mine]

    def scattered(which, got, c):
        skip = 1 if c == 0 else 0
        settle(got.at[pl.ds(2 * c + skip, 2 - skip)], a2a_rs.at[which, c])

    for load in loads[:3]:
        load.wait()
    for load in loads[3:]:
        load.start()
    pack(dot(hid[...], wk[...]) * scale, val[...], kv_s)
    pl.semaphore_wait(barrier, n - 1)
    scatter(0, kv_s, kv_a)
    for load in loads[3:5]:
        load.wait()
    pack(dot(hid[...], wq[...]) * scale, gout[...], qg_s)
    scatter(1, qg_s, qg_a)

    for h in range(2):
        for q in range(parts):
            spot = pl.multiple_of(h * half + order[q] * LANES, LANES)
            hid_f[h, q] = hid[:, pl.ds(spot, LANES)].astype(F32)

    relayed = [m for m in range(1, groups) if m & 6 == 6 and m < 8]
    direct = [m for m in range(1, groups) if m not in relayed]
    passed_on = [2, 5] if relayed else []
    ahead = 2

    def hidden_start(q, m):
        if m in relayed:
            via, hop = (2, 4) if m == 6 else (5, 2)
            source, to = hid_r.at[q, via], flipped(me, hop)
        else:
            to = flipped(me, m)
            source = hid_f.at[to % 2, q]
        recv = hid_rs.at[q, 1 if m in passed_on else 0]
        remote(source, hid_r.at[q, m], hid_ss.at[0], recv, to).start()

    def send_hidden(q):
        if q < parts:
            for m in passed_on + [m for m in direct if m not in passed_on]:
                hidden_start(q, m)
            hid_r[q, 0] = hid_f[core, q]

    for q in range(ahead):
        send_hidden(q)

    def relay(q):
        if q < parts:
            if passed_on:
                settle(hid_r.at[q, pl.ds(0, len(passed_on))], hid_rs.at[q, 1])
            for m in relayed:
                hidden_start(q, m)
            send_hidden(q + ahead)

    def hidden_rows(q):
        settle(hid_r.at[q, pl.ds(0, groups - 1 - len(passed_on))], hid_rs.at[q, 0])
        return hid_r[q].reshape(groups * toks, LANES).astype(BF16)

    loads[5].wait()
    for j in range(groups):
        rf_high, rf_low = halves(rf[j])
        rfs[j] = jnp.concatenate([rf_high, rf_high, rf_low, rf_low], axis=0)
        rbs[j] = jnp.concatenate([rf_high, rf_low], axis=0)

    def features(x, j):
        rows = jnp.where(low(x.shape), x, 0.0)
        high = rows.astype(BF16).astype(F32)
        both = (high + swap(rows - high)).astype(BF16)
        logits = dot(jnp.concatenate([both, both], axis=1), rfs[j])
        return jnp.exp(logits - 0.5 * jnp.sum(rows * rows, axis=1, keepdims=True)) * norm

    def chunk(ref, c):
        return ref[2 * c : 2 * c + 2].reshape(2 * toks, ref.shape[2])

    def folded(total):
        slabs = [total[:, s : s + LANES] for s in range(0, feats, LANES)]
        return jnp.concatenate([t[head_dim:] for t in slabs] + [t[:1] for t in slabs], axis=0)

    def spread(packed):
        count = feats // LANES
        rows = jnp.concatenate(
            [packed[i * head_dim : (i + 1) * head_dim] for i in range(count)], axis=1
        )
        base = count * head_dim
        z = jnp.concatenate([packed[base + i : base + i + 1] for i in range(count)], axis=1)
        return halves(
            jnp.concatenate([jnp.broadcast_to(z, (head_dim, feats)), rows], axis=0)
        )

    def all_reduce(which, total):
        packed = folded(total)
        stride = groups
        for f, radix in enumerate(phases):
            ar_s[which, f] = packed
            for d in range(1, radix):
                remote(
                    ar_s.at[which, f], ar_r.at[which, f, d - 1],
                    ar_ss.at[which, f], ar_rs.at[which, f], flipped(me, d, stride),
                ).start()
            yield
            came = ar_r.at[which, f, pl.ds(0, radix - 1)]
            settle(came, ar_rs.at[which, f])
            settle(came, ar_ss.at[which, f])
            for d in range(radix - 1):
                packed = packed + ar_r[which, f, d]
            stride *= radix
        yield packed

    def finish(steps):
        for got in steps:
            if got is not None:
                return got

    for j in range(groups):
        feat_l[j] = features(kv_s[j], j)

    total = jnp.zeros((LANES, feats), F32)
    for c in range(pairs):
        scattered(0, kv_a, c)
        x = chunk(kv_a, c)
        b = features(x, mine)
        feat_k[c] = b
        high, rest = halves(b)
        ones = jnp.where(low(x.shape), 1.0, x).T.astype(BF16)
        total = total + dot(ones, high) + dot(ones, rest)
    reduce_k = all_reduce(0, total)
    next(reduce_k)

    for c in range(pairs):
        scattered(1, qg_a, c)
        a = features(chunk(qg_a, c), mine)
        feat_q[c] = a
        feat_h[0, c], feat_h[1, c] = halves(a)

    st_high, st_low = spread(finish(reduce_k))
    st_both = jnp.concatenate([st_high, st_low], axis=0)
    total = jnp.zeros((LANES, feats), F32)
    for c in range(pairs):
        x = chunk(qg_a, c)
        high, rest = feat_h[0, c], feat_h[1, c]
        nd = dot_t(high, st_both)
        nd = nd[:, :LANES] + nd[:, LANES:] + dot_t(rest, st_high)
        mask = low(nd.shape)
        inverse = 1.0 / jnp.where(mask, nd, swap(nd))
        upstream = jnp.where(mask, 0.0, x) * inverse
        grad_den = -jnp.sum(upstream * (nd * inverse), axis=1, keepdims=True)
        lane = lax.broadcasted_iota(jnp.int32, nd.shape, 1)
        xg = jnp.where(lane == 0, grad_den, upstream)
        bwd_x[c] = xg
        turned_high, turned_low = halves(xg.T)
        total = total + dot(turned_high, high) + dot(turned_low, high) + dot(turned_high, rest)
    reduce_q = all_reduce(1, total)
    next(reduce_q)
    relay(0)

    def feature_grad(x, weighted, j):
        high, rest = halves(weighted)
        back = dot_t(high, rbs[j]) + dot_t(rest, rbs[j])
        back = back + swap(back)
        out = (back - x * jnp.sum(weighted, axis=1, keepdims=True)) * scale
        return jnp.where(low(x.shape), out.astype(BF16).astype(F32), 0.0)

    def pair_send(which, outs):
        for c, out in outs:
            pair_s[which, c] = out[:toks] + swap(out[toks:])
        for c, _ in outs:
            remote(
                pair_s.at[which, c], pair_r.at[which, c],
                pair_ss.at[which], pair_rs.at[which, c], partner,
            ).start()

    def paired(which, c):
        settle(pair_r.at[which, c], pair_rs.at[which, c])
        own, theirs = pair_s[which, c], pair_r[which, c]
        mask = low(own.shape)
        for m, a, b in ((2 * c, own, swap(theirs)), (2 * c + 1, swap(own), theirs)):
            both = jnp.where(first, jnp.where(mask, a, swap(b)), jnp.where(mask, b, swap(a)))
            turned[which, :, m * toks : (m + 1) * toks] = both.T.astype(BF16)
            if which == 0:
                dq_p[m] = both

    def query_grad(c):
        x = chunk(qg_a, c)
        high, rest = halves(bwd_x[c])
        grads = dot(
            jnp.concatenate([high, rest], axis=1), jnp.concatenate([st_high, st_high], axis=0)
        ) + dot(high, st_low)
        return c, feature_grad(x, feat_q[c] * grads, mine)

    for c in range(0, pairs, 2):
        pair_send(0, [query_grad(c), query_grad(c + 1)])

    relay(1)
    for c in range(pairs):
        paired(0, c)

    def weight_part(which, q, rows):
        total = dot(turned[which], rows).T.reshape(per, block, LANES)
        if q < later:
            gw_s[which, q] = total
            remote(
                gw_s.at[which, q], gw_x.at[which, q], gw_ss.at[2], gw_xs.at[which, q], plane_next
            ).start()
            return
        settle(gw_x.at[which, q - later], gw_xs.at[which, q - later])
        gw_s[which, q] = total + gw_x[which, q - later]
        slot = (me // groups) // 2 * pairs + pair

        def start(i, carry):
            to = core * (n // 2) + order[q] * per + i

            @pl.when(to != me)
            def _():
                remote(
                    gw_s.at[which, q, i], gw_r.at[which, slot], gw_ss.at[which], gw_rs.at[which], to
                ).start()

            @pl.when(to == me)
            def _():
                pltpu.make_async_copy(
                    gw_s.at[which, q, i], gw_r.at[which, slot], gw_rs.at[which]
                ).start()

            return carry

        lax.fori_loop(0, per, start, 0)

    relay(2)
    weight_part(0, 0, hidden_rows(0))

    total = finish(reduce_q)
    states[mine] = total

    def state_send(to, slot, which):
        remote(states.at[slot], states.at[slot], st_ss.at[0], st_rs.at[which], to).start()


    def value_rows(x):
        lane = lax.broadcasted_iota(jnp.int32, x.shape, 1)
        ones = jnp.where(lane == 0, 1.0, 0.0)
        xv = jnp.where(low(x.shape), ones, x).astype(BF16)
        return jnp.concatenate([xv, xv], axis=1)

    gs_high, gs_low = spread(total)
    gs_both = jnp.concatenate([gs_high, gs_low], axis=0)

    def key_grad(c):
        x = chunk(kv_a, c)
        return c, feature_grad(x, feat_k[c] * dot(value_rows(x), gs_both), mine)

    for c in range(0, pairs, 2):
        pair_send(1, [key_grad(c), key_grad(c + 1)])
    relay(3)
    for m in range(2, groups, 2):
        state_send(flipped(me, m), mine, 0)
    state_send(partner, mine, 1)
    weight_part(0, 1, hidden_rows(1))
    for c in range(pairs):
        paired(1, c)
    for q in range(later):
        weight_part(1, q, hid_r[q].reshape(groups * toks, LANES).astype(BF16))
    for m in range(2, groups, 2):
        remote(
            dq_p.at[m], dq_a.at[pair], back_ss.at[0], back_rs.at[0], flipped(me, m)
        ).start()
    dq_a[pair] = dq_p[0]
    for q in range(later, parts):
        if q > 2:
            relay(q + 1)
        weight_part(0, q, hidden_rows(q))
    for q in range(later, parts):
        weight_part(1, q, hid_r[q].reshape(groups * toks, LANES).astype(BF16))

    if pairs > 1:
        settle(states.at[pl.ds(0, pairs - 1)], st_rs.at[0])
    for m in range(2, groups, 2):
        state_send(partner, flipped(me, m) % groups, 1)
    settle(states.at[pl.ds(0, pairs)], st_rs.at[1])
    dk_slabs = []
    for p in range(pairs):
        outs = []
        for j in (2 * p, 2 * p + 1):
            gs_high, gs_low = spread(states[j])
            gs_both = jnp.concatenate([gs_high, gs_low], axis=0)
            x, b = kv_s[j], feat_l[j]
            out = feature_grad(x, b * dot(value_rows(x), gs_both), j)
            high, rest = halves(b)
            gv = dot_t(high, gs_both)
            gv = gv[:, :LANES] + gv[:, LANES:] + dot_t(rest, gs_high)
            outs.append((out, gv))
        (dk_one, gv_one), (dk_two, gv_two) = outs
        mask = low(dk_one.shape)
        dk_slabs.append(jnp.where(mask, dk_one, swap(dk_two)))
        slab = jnp.where(mask, swap(gv_one), gv_two)
        o_val[:, p * LANES : (p + 1) * LANES] = slab.astype(BF16)
    o_hid[...] = dot_t(jnp.concatenate(dk_slabs, axis=1).astype(BF16), wk[...])
    settle(dq_a.at[pl.ds(0, pairs - 1)], back_rs.at[0])
    dq_all = jnp.concatenate([dq_a[p] for p in range(pairs)], axis=1).astype(BF16)
    o_hid[...] += dot_t(dq_all, wq[...])

    for which in range(2):
        settle(gw_r.at[which], gw_rs.at[which])
    for which, out in ((0, o_gq), (1, o_gk)):
        for p in range(pairs):
            total = gw_r[which, p]
            for i in range(p + pairs, n // 4, pairs):
                total = total + gw_r[which, i]
            out[:, p * LANES : (p + 1) * LANES] = total
    for which in range(2):
        others = kv_a.at[pl.ds(1, groups - 1)]
        settle(others, a2a_ss.at[which])
        settle(pair_s.at[which], pair_ss.at[which])
        own_set = me // (n // 4) == 2 * core + parity

        @pl.when(own_set)
        def _():
            settle(gw_r.at[which, pl.ds(0, n // 4 - 1)], gw_ss.at[which])

        @pl.when(jnp.logical_not(own_set))
        def _():
            settle(gw_r.at[which], gw_ss.at[which])

    settle(gw_x, gw_ss.at[2])
    settle(dq_a.at[pl.ds(0, pairs - 1)], back_ss.at[0])
    settle(states.at[pl.ds(0, groups - 1)], st_ss.at[0])
    settle(hid_r.at[:, pl.ds(1, groups - 1)], hid_ss.at[0])


def store(*refs):
    count = len(refs) // 2
    sems = refs[-1]
    copies = [
        pltpu.make_async_copy(refs[i], refs[count + i], sems.at[i]) for i in range(count)
    ]
    for copy in copies:
        copy.start()
    for copy in copies:
        copy.wait()


def shards(n, *args):
    hidden, random_feats = args[0], args[5]
    toks, width = hidden.shape
    groups, head_dim, feats = random_feats.shape
    cols = groups * head_dim
    pairs = groups // 2
    block = width // n
    parts = width // 2 // LANES
    phases = len(radices(n // groups))
    rows = (head_dim + 1) * feats // LANES
    tok_block = (groups, toks, LANES)
    scratch = [pltpu.VMEM(a.shape, a.dtype) for a in args]
    scratch += [
        pltpu.VMEM((2, parts, toks, LANES), F32),
        pltpu.VMEM((parts,) + tok_block, F32),
    ]
    scratch += [pltpu.VMEM(tok_block, F32)] * 4
    scratch += [
        pltpu.VMEM((groups, 4 * head_dim, feats), BF16),
        pltpu.VMEM((groups, 2 * head_dim, feats), BF16),
        pltpu.VMEM((pairs, 2 * toks, feats), F32),
        pltpu.VMEM((pairs, 2 * toks, feats), F32),
        pltpu.VMEM((2, pairs, 2 * toks, feats), BF16),
        pltpu.VMEM((pairs, 2 * toks, LANES), F32),
        pltpu.VMEM((2, phases, rows, LANES), F32),
        pltpu.VMEM((2, phases, 3, rows, LANES), F32),
    ]
    scratch += [pltpu.VMEM((2, pairs, toks, LANES), F32)] * 2
    scratch += [
        pltpu.VMEM(tok_block, F32),
        pltpu.VMEM((2, LANES, groups * toks), BF16),
        pltpu.VMEM((groups, toks, feats), F32),
        pltpu.VMEM((groups, rows, LANES), F32),
        pltpu.VMEM((pairs, toks, LANES), F32),
    ]
    scratch += [
        pltpu.VMEM((2, parts, LANES // block, block, LANES), F32),
        pltpu.VMEM((2, parts // 2, LANES // block, block, LANES), F32),
        pltpu.VMEM((2, n // 4, block, LANES), F32),
    ]
    for shape in (
        (6,), (2,), (2, pairs), (1,), (parts, 2), (2, phases), (2, phases), (2,), (2, pairs),
        (1,), (1,), (1,), (2,), (3,), (2, parts // 2), (2,),
    ):
        scratch.append(pltpu.SemaphoreType.DMA(shape))
    vmem = pl.BlockSpec(memory_space=pltpu.VMEM)
    anywhere = pl.BlockSpec(memory_space=pl.ANY)
    shapes = (
        jax.ShapeDtypeStruct((toks, width), F32),
        jax.ShapeDtypeStruct((toks, cols), BF16),
        jax.ShapeDtypeStruct((block, cols), F32),
        jax.ShapeDtypeStruct((block, cols), F32),
    )
    out = pl.pallas_call(
        functools.partial(kernel, n),
        out_shape=tuple(pltpu.VMEM(a.shape, a.dtype) for a in shapes),
        in_specs=[anywhere] * 6,
        out_specs=(vmem,) * 4,
        scratch_shapes=scratch,
        compiler_params=pltpu.CompilerParams(
            collective_id=0, has_side_effects=True, vmem_limit_bytes=56 * 2**20
        ),
        name="backward",
    )(*args)
    return pl.pallas_call(
        store,
        out_shape=shapes,
        in_specs=[vmem] * 4,
        out_specs=(anywhere,) * 4,
        scratch_shapes=[pltpu.SemaphoreType.DMA((4,))],
        name="store",
    )(*[pltpu.with_memory_space_constraint(a, pltpu.VMEM) for a in out])


def solution(mesh):
    placed = (
        P("seq", None),
        P(None, "head"),
        P(None, "head"),
        P("seq", "head"),
        P("seq", "head"),
        P("head", None, None),
    )

    def local(*args):
        out = shards(mesh.shape["seq"], *args)
        if mesh.shape["head"] == 1:
            return out
        return (lax.psum(out[0], "head"),) + tuple(out[1:])

    return jax.shard_map(
        local,
        mesh=mesh,
        in_specs=placed,
        out_specs=(P("seq", None), P("seq", "head"), P("seq", "head"), P("seq", "head")),
        check_vma=False,
    )
```

```python
import functools

import jax
import jax.numpy as jnp
from jax import lax
from jax.experimental import pallas as pl
from jax.experimental.pallas import tpu as pltpu
from jax.sharding import PartitionSpec as P

F32, BF16 = jnp.float32, jnp.bfloat16
LANES = 128
MESH = pl.DeviceIdType.MESH


def flipped(index, mask, stride=1):
    out, b = index, 0
    while mask >> b:
        if (mask >> b) & 1:
            bit = (index // (stride * 2**b)) % 2
            out = out + (1 - 2 * bit) * (stride * 2**b)
        b += 1
    return out


def radices(count):
    out = []
    while count > 1:
        out.append(4 if count % 4 == 0 else 2)
        count //= out[-1]
    return out


def dot(a, b):
    return jnp.dot(a, b, preferred_element_type=F32)


def dot_t(a, b):
    return lax.dot_general(a, b, (((1,), (1,)), ((), ())), preferred_element_type=F32)


def halves(x):
    high = x.astype(BF16)
    return high, (x - high.astype(F32)).astype(BF16)


def swap(x):
    return pltpu.roll(x, LANES // 2, 1)


def settle(ref, sem):
    pltpu.make_async_copy(ref, ref, sem).wait()


def remote(src, dst, send_sem, recv_sem, peer):
    return pltpu.make_async_remote_copy(
        src_ref=src, dst_ref=dst, send_sem=send_sem, recv_sem=recv_sem,
        device_id={"seq": peer}, device_id_type=MESH,
    )


def kernel(
    n, hid_h, wq_h, wk_h, val_h, gout_h, rf_h, o_hid, o_val, o_gq, o_gk,
    hid, wq, wk, val, gout, rf,
    hid_f, hid_r, kv_s, kv_a, qg_s, qg_a, rfs, rbs, feat_k, feat_q, feat_h, bwd_x,
    ar_s, ar_r, pair_s, pair_r, dq_p, turned, feat_l, states, dq_a, gw_s, gw_x, gw_r,
    in_ss, a2a_ss, a2a_rs, hid_ss, hid_rs, ar_ss, ar_rs, pair_ss, pair_rs, back_ss, back_rs,
    st_ss, st_rs, gw_ss, gw_xs, gw_rs,
):
    groups, head_dim, feats = rf.shape
    toks, width = hid.shape
    half = width // 2
    parts = half // LANES
    block = gw_s.shape[3]
    per = LANES // block
    later = parts // 2
    pairs = groups // 2
    scale = head_dim ** (-0.25)
    norm = feats ** (-0.5)
    me = lax.axis_index("seq")
    mine = me % groups
    core = me % 2
    pair = mine // 2
    first = core == 0
    phases = radices(n // groups)
    partner = flipped(me, 1)
    parity = (me // groups) % 2
    plane_next = flipped(me, 1, groups)
    order = [(i + (1 - parity) * later) % parts for i in range(parts)]

    barrier = pltpu.get_barrier_semaphore()

    def greet(step, carry):
        pl.semaphore_signal(
            barrier, inc=1, device_id={"seq": (me + step) % n}, device_id_type=MESH
        )
        return carry

    loads = []
    for i, (src, dst) in enumerate(
        [(hid_h, hid), (wk_h, wk), (val_h, val), (wq_h, wq), (gout_h, gout), (rf_h, rf)]
    ):
        loads.append(pltpu.make_async_copy(src, dst, in_ss.at[i]))
    for load in loads[:3]:
        load.start()
    lax.fori_loop(1, n, greet, 0)

    def low(shape):
        return lax.broadcasted_iota(jnp.int32, shape, 1) < head_dim

    def pack(proj, other, out):
        for p in range(pairs):
            a = proj[:, p * LANES : (p + 1) * LANES]
            b = other[:, p * LANES : (p + 1) * LANES].astype(F32)
            mask = low(a.shape)
            out[2 * p] = jnp.where(mask, a, swap(b))
            out[2 * p + 1] = jnp.where(mask, swap(a), b)

    def scatter(which, sent, got):
        for m in range(1, groups):
            to = flipped(me, m)
            remote(
                sent.at[to % groups], got.at[m], a2a_ss.at[which], a2a_rs.at[which, m // 2], to
            ).start()
        got[0] = sent[mine]

    def scattered(which, got, c):
        skip = 1 if c == 0 else 0
        settle(got.at[pl.ds(2 * c + skip, 2 - skip)], a2a_rs.at[which, c])

    for load in loads[:3]:
        load.wait()
    for load in loads[3:]:
        load.start()
    pack(dot(hid[...], wk[...]) * scale, val[...], kv_s)
    pl.semaphore_wait(barrier, n - 1)
    scatter(0, kv_s, kv_a)
    for load in loads[3:5]:
        load.wait()
    pack(dot(hid[...], wq[...]) * scale, gout[...], qg_s)
    scatter(1, qg_s, qg_a)

    for h in range(2):
        for q in range(parts):
            spot = pl.multiple_of(h * half + order[q] * LANES, LANES)
            hid_f[h, q] = hid[:, pl.ds(spot, LANES)].astype(F32)

    relayed = [m for m in range(1, groups) if m & 6 == 6 and m < 8]
    direct = [m for m in range(1, groups) if m not in relayed]
    passed_on = [2, 5] if relayed else []
    ahead = 3

    def hidden_start(q, m):
        if m in relayed:
            via, hop = (2, 4) if m == 6 else (5, 2)
            source, to = hid_r.at[q, via], flipped(me, hop)
        else:
            to = flipped(me, m)
            source = hid_f.at[to % 2, q]
        recv = hid_rs.at[q, 1 if m in passed_on else 0]
        remote(source, hid_r.at[q, m], hid_ss.at[0], recv, to).start()

    def send_hidden(q):
        if q < parts:
            for m in passed_on + [m for m in direct if m not in passed_on]:
                hidden_start(q, m)
            hid_r[q, 0] = hid_f[core, q]

    for q in range(ahead):
        send_hidden(q)

    def relay(q):
        if q < parts:
            if passed_on:
                settle(hid_r.at[q, pl.ds(0, len(passed_on))], hid_rs.at[q, 1])
            for m in relayed:
                hidden_start(q, m)
            send_hidden(q + ahead)

    def hidden_rows(q):
        settle(hid_r.at[q, pl.ds(0, groups - 1 - len(passed_on))], hid_rs.at[q, 0])
        return hid_r[q].reshape(groups * toks, LANES).astype(BF16)

    loads[5].wait()
    for j in range(groups):
        rf_high, rf_low = halves(rf[j])
        rfs[j] = jnp.concatenate([rf_high, rf_high, rf_low, rf_low], axis=0)
        rbs[j] = jnp.concatenate([rf_high, rf_low], axis=0)

    def features(x, j):
        rows = jnp.where(low(x.shape), x, 0.0)
        high = rows.astype(BF16).astype(F32)
        both = (high + swap(rows - high)).astype(BF16)
        logits = dot(jnp.concatenate([both, both], axis=1), rfs[j])
        return jnp.exp(logits - 0.5 * jnp.sum(rows * rows, axis=1, keepdims=True)) * norm

    def chunk(ref, c):
        return ref[2 * c : 2 * c + 2].reshape(2 * toks, ref.shape[2])

    def folded(total):
        slabs = [total[:, s : s + LANES] for s in range(0, feats, LANES)]
        return jnp.concatenate([t[head_dim:] for t in slabs] + [t[:1] for t in slabs], axis=0)

    def spread(packed):
        count = feats // LANES
        rows = jnp.concatenate(
            [packed[i * head_dim : (i + 1) * head_dim] for i in range(count)], axis=1
        )
        base = count * head_dim
        z = jnp.concatenate([packed[base + i : base + i + 1] for i in range(count)], axis=1)
        return halves(
            jnp.concatenate([jnp.broadcast_to(z, (head_dim, feats)), rows], axis=0)
        )

    def all_reduce(which, total):
        packed = folded(total)
        stride = groups
        for f, radix in enumerate(phases):
            ar_s[which, f] = packed
            for d in range(1, radix):
                remote(
                    ar_s.at[which, f], ar_r.at[which, f, d - 1],
                    ar_ss.at[which, f], ar_rs.at[which, f], flipped(me, d, stride),
                ).start()
            yield
            came = ar_r.at[which, f, pl.ds(0, radix - 1)]
            settle(came, ar_rs.at[which, f])
            settle(came, ar_ss.at[which, f])
            for d in range(radix - 1):
                packed = packed + ar_r[which, f, d]
            stride *= radix
        yield packed

    def finish(steps):
        for got in steps:
            if got is not None:
                return got

    for j in range(groups):
        feat_l[j] = features(kv_s[j], j)

    total = jnp.zeros((LANES, feats), F32)
    for c in range(pairs):
        scattered(0, kv_a, c)
        x = chunk(kv_a, c)
        b = features(x, mine)
        feat_k[c] = b
        high, rest = halves(b)
        ones = jnp.where(low(x.shape), 1.0, x).T.astype(BF16)
        total = total + dot(ones, high) + dot(ones, rest)
    reduce_k = all_reduce(0, total)
    next(reduce_k)

    for c in range(pairs):
        scattered(1, qg_a, c)
        a = features(chunk(qg_a, c), mine)
        feat_q[c] = a
        feat_h[0, c], feat_h[1, c] = halves(a)

    st_high, st_low = spread(finish(reduce_k))
    st_both = jnp.concatenate([st_high, st_low], axis=0)
    total = jnp.zeros((LANES, feats), F32)
    for c in range(pairs):
        x = chunk(qg_a, c)
        high, rest = feat_h[0, c], feat_h[1, c]
        nd = dot_t(high, st_both)
        nd = nd[:, :LANES] + nd[:, LANES:] + dot_t(rest, st_high)
        mask = low(nd.shape)
        inverse = 1.0 / jnp.where(mask, nd, swap(nd))
        upstream = jnp.where(mask, 0.0, x) * inverse
        grad_den = -jnp.sum(upstream * (nd * inverse), axis=1, keepdims=True)
        lane = lax.broadcasted_iota(jnp.int32, nd.shape, 1)
        xg = jnp.where(lane == 0, grad_den, upstream)
        bwd_x[c] = xg
        turned_high, turned_low = halves(xg.T)
        total = total + dot(turned_high, high) + dot(turned_low, high) + dot(turned_high, rest)
    reduce_q = all_reduce(1, total)
    next(reduce_q)
    relay(0)

    def feature_grad(x, weighted, j):
        high, rest = halves(weighted)
        back = dot_t(high, rbs[j]) + dot_t(rest, rbs[j])
        back = back + swap(back)
        out = (back - x * jnp.sum(weighted, axis=1, keepdims=True)) * scale
        return jnp.where(low(x.shape), out.astype(BF16).astype(F32), 0.0)

    def pair_send(which, outs):
        for c, out in outs:
            pair_s[which, c] = out[:toks] + swap(out[toks:])
        for c, _ in outs:
            remote(
                pair_s.at[which, c], pair_r.at[which, c],
                pair_ss.at[which], pair_rs.at[which, c], partner,
            ).start()

    def paired(which, c):
        settle(pair_r.at[which, c], pair_rs.at[which, c])
        own, theirs = pair_s[which, c], pair_r[which, c]
        mask = low(own.shape)
        for m, a, b in ((2 * c, own, swap(theirs)), (2 * c + 1, swap(own), theirs)):
            both = jnp.where(first, jnp.where(mask, a, swap(b)), jnp.where(mask, b, swap(a)))
            turned[which, :, m * toks : (m + 1) * toks] = both.T.astype(BF16)
            if which == 0:
                dq_p[m] = both

    def query_grad(c):
        x = chunk(qg_a, c)
        high, rest = halves(bwd_x[c])
        grads = dot(
            jnp.concatenate([high, rest], axis=1), jnp.concatenate([st_high, st_high], axis=0)
        ) + dot(high, st_low)
        return c, feature_grad(x, feat_q[c] * grads, mine)

    for c in range(0, pairs, 2):
        pair_send(0, [query_grad(c), query_grad(c + 1)])

    relay(1)
    for c in range(pairs):
        paired(0, c)

    def weight_part(which, q, rows):
        total = dot(turned[which], rows).T.reshape(per, block, LANES)
        if q < later:
            gw_s[which, q] = total
            remote(
                gw_s.at[which, q], gw_x.at[which, q], gw_ss.at[2], gw_xs.at[which, q], plane_next
            ).start()
            return
        settle(gw_x.at[which, q - later], gw_xs.at[which, q - later])
        gw_s[which, q] = total + gw_x[which, q - later]
        slot = (me // groups) // 2 * pairs + pair

        def start(i, carry):
            to = core * (n // 2) + order[q] * per + i

            @pl.when(to != me)
            def _():
                remote(
                    gw_s.at[which, q, i], gw_r.at[which, slot], gw_ss.at[which], gw_rs.at[which], to
                ).start()

            @pl.when(to == me)
            def _():
                pltpu.make_async_copy(
                    gw_s.at[which, q, i], gw_r.at[which, slot], gw_rs.at[which]
                ).start()

            return carry

        lax.fori_loop(0, per, start, 0)

    relay(2)
    weight_part(0, 0, hidden_rows(0))

    total = finish(reduce_q)
    states[mine] = total

    def state_send(to, slot, which):
        remote(states.at[slot], states.at[slot], st_ss.at[0], st_rs.at[which], to).start()


    def value_rows(x):
        lane = lax.broadcasted_iota(jnp.int32, x.shape, 1)
        ones = jnp.where(lane == 0, 1.0, 0.0)
        xv = jnp.where(low(x.shape), ones, x).astype(BF16)
        return jnp.concatenate([xv, xv], axis=1)

    gs_high, gs_low = spread(total)
    gs_both = jnp.concatenate([gs_high, gs_low], axis=0)

    def key_grad(c):
        x = chunk(kv_a, c)
        return c, feature_grad(x, feat_k[c] * dot(value_rows(x), gs_both), mine)

    for c in range(0, pairs, 2):
        pair_send(1, [key_grad(c), key_grad(c + 1)])
    relay(3)
    for m in range(2, groups, 2):
        state_send(flipped(me, m), mine, 0)
    state_send(partner, mine, 1)
    weight_part(0, 1, hidden_rows(1))
    for c in range(pairs):
        paired(1, c)
    for q in range(later):
        weight_part(1, q, hid_r[q].reshape(groups * toks, LANES).astype(BF16))
    for m in range(2, groups, 2):
        remote(
            dq_p.at[m], dq_a.at[pair], back_ss.at[0], back_rs.at[0], flipped(me, m)
        ).start()
    dq_a[pair] = dq_p[0]
    for q in range(later, parts):
        if q > 2:
            relay(q + 1)
        weight_part(0, q, hidden_rows(q))
    for q in range(later, parts):
        weight_part(1, q, hid_r[q].reshape(groups * toks, LANES).astype(BF16))

    if pairs > 1:
        settle(states.at[pl.ds(0, pairs - 1)], st_rs.at[0])
    for m in range(2, groups, 2):
        state_send(partner, flipped(me, m) % groups, 1)

    def own_grads(j):
        gs_high, gs_low = spread(states[j])
        gs_both = jnp.concatenate([gs_high, gs_low], axis=0)
        x, b = kv_s[j], feat_l[j]
        out = feature_grad(x, b * dot(value_rows(x), gs_both), j)
        high, rest = halves(b)
        gv = dot_t(high, gs_both)
        return out, gv[:, :LANES] + gv[:, LANES:] + dot_t(rest, gs_high)

    here = [own_grads(2 * p + core) for p in range(pairs)]
    settle(states.at[pl.ds(0, pairs)], st_rs.at[1])
    there = [own_grads(2 * p + 1 - core) for p in range(pairs)]
    dk_slabs = []
    for p, ((dk_own, gv_own), (dk_other, gv_other)) in enumerate(zip(here, there)):
        mask = low(dk_own.shape)
        dk_one, dk_two = jnp.where(first, dk_own, dk_other), jnp.where(first, dk_other, dk_own)
        gv_one, gv_two = jnp.where(first, gv_own, gv_other), jnp.where(first, gv_other, gv_own)
        dk_slabs.append(jnp.where(mask, dk_one, swap(dk_two)))
        slab = jnp.where(mask, swap(gv_one), gv_two)
        o_val[:, p * LANES : (p + 1) * LANES] = slab.astype(BF16)
    o_hid[...] = dot_t(jnp.concatenate(dk_slabs, axis=1).astype(BF16), wk[...])
    settle(dq_a.at[pl.ds(0, pairs - 1)], back_rs.at[0])
    dq_all = jnp.concatenate([dq_a[p] for p in range(pairs)], axis=1).astype(BF16)
    o_hid[...] += dot_t(dq_all, wq[...])

    for which in range(2):
        settle(gw_r.at[which], gw_rs.at[which])
    for which, out in ((0, o_gq), (1, o_gk)):
        for p in range(pairs):
            total = gw_r[which, p]
            for i in range(p + pairs, n // 4, pairs):
                total = total + gw_r[which, i]
            out[:, p * LANES : (p + 1) * LANES] = total
    for which in range(2):
        others = kv_a.at[pl.ds(1, groups - 1)]
        settle(others, a2a_ss.at[which])
        settle(pair_s.at[which], pair_ss.at[which])
        own_set = me // (n // 4) == 2 * core + parity

        @pl.when(own_set)
        def _():
            settle(gw_r.at[which, pl.ds(0, n // 4 - 1)], gw_ss.at[which])

        @pl.when(jnp.logical_not(own_set))
        def _():
            settle(gw_r.at[which], gw_ss.at[which])

    settle(gw_x, gw_ss.at[2])
    settle(dq_a.at[pl.ds(0, pairs - 1)], back_ss.at[0])
    settle(states.at[pl.ds(0, groups - 1)], st_ss.at[0])
    settle(hid_r.at[:, pl.ds(1, groups - 1)], hid_ss.at[0])


def store(*refs):
    count = len(refs) // 2
    sems = refs[-1]
    copies = [
        pltpu.make_async_copy(refs[i], refs[count + i], sems.at[i]) for i in range(count)
    ]
    for copy in copies:
        copy.start()
    for copy in copies:
        copy.wait()


def shards(n, *args):
    hidden, random_feats = args[0], args[5]
    toks, width = hidden.shape
    groups, head_dim, feats = random_feats.shape
    cols = groups * head_dim
    pairs = groups // 2
    block = width // n
    parts = width // 2 // LANES
    phases = len(radices(n // groups))
    rows = (head_dim + 1) * feats // LANES
    tok_block = (groups, toks, LANES)
    scratch = [pltpu.VMEM(a.shape, a.dtype) for a in args]
    scratch += [
        pltpu.VMEM((2, parts, toks, LANES), F32),
        pltpu.VMEM((parts,) + tok_block, F32),
    ]
    scratch += [pltpu.VMEM(tok_block, F32)] * 4
    scratch += [
        pltpu.VMEM((groups, 4 * head_dim, feats), BF16),
        pltpu.VMEM((groups, 2 * head_dim, feats), BF16),
        pltpu.VMEM((pairs, 2 * toks, feats), F32),
        pltpu.VMEM((pairs, 2 * toks, feats), F32),
        pltpu.VMEM((2, pairs, 2 * toks, feats), BF16),
        pltpu.VMEM((pairs, 2 * toks, LANES), F32),
        pltpu.VMEM((2, phases, rows, LANES), F32),
        pltpu.VMEM((2, phases, 3, rows, LANES), F32),
    ]
    scratch += [pltpu.VMEM((2, pairs, toks, LANES), F32)] * 2
    scratch += [
        pltpu.VMEM(tok_block, F32),
        pltpu.VMEM((2, LANES, groups * toks), BF16),
        pltpu.VMEM((groups, toks, feats), F32),
        pltpu.VMEM((groups, rows, LANES), F32),
        pltpu.VMEM((pairs, toks, LANES), F32),
    ]
    scratch += [
        pltpu.VMEM((2, parts, LANES // block, block, LANES), F32),
        pltpu.VMEM((2, parts // 2, LANES // block, block, LANES), F32),
        pltpu.VMEM((2, n // 4, block, LANES), F32),
    ]
    for shape in (
        (6,), (2,), (2, pairs), (1,), (parts, 2), (2, phases), (2, phases), (2,), (2, pairs),
        (1,), (1,), (1,), (2,), (3,), (2, parts // 2), (2,),
    ):
        scratch.append(pltpu.SemaphoreType.DMA(shape))
    vmem = pl.BlockSpec(memory_space=pltpu.VMEM)
    anywhere = pl.BlockSpec(memory_space=pl.ANY)
    shapes = (
        jax.ShapeDtypeStruct((toks, width), F32),
        jax.ShapeDtypeStruct((toks, cols), BF16),
        jax.ShapeDtypeStruct((block, cols), F32),
        jax.ShapeDtypeStruct((block, cols), F32),
    )
    out = pl.pallas_call(
        functools.partial(kernel, n),
        out_shape=tuple(pltpu.VMEM(a.shape, a.dtype) for a in shapes),
        in_specs=[anywhere] * 6,
        out_specs=(vmem,) * 4,
        scratch_shapes=scratch,
        compiler_params=pltpu.CompilerParams(
            collective_id=0, has_side_effects=True, vmem_limit_bytes=56 * 2**20
        ),
        name="backward",
    )(*args)
    return pl.pallas_call(
        store,
        out_shape=shapes,
        in_specs=[vmem] * 4,
        out_specs=(anywhere,) * 4,
        scratch_shapes=[pltpu.SemaphoreType.DMA((4,))],
        name="store",
    )(*[pltpu.with_memory_space_constraint(a, pltpu.VMEM) for a in out])


def solution(mesh):
    placed = (
        P("seq", None),
        P(None, "head"),
        P(None, "head"),
        P("seq", "head"),
        P("seq", "head"),
        P("head", None, None),
    )

    def local(*args):
        out = shards(mesh.shape["seq"], *args)
        if mesh.shape["head"] == 1:
            return out
        return (lax.psum(out[0], "head"),) + tuple(out[1:])

    return jax.shard_map(
        local,
        mesh=mesh,
        in_specs=placed,
        out_specs=(P("seq", None), P("seq", "head"), P("seq", "head"), P("seq", "head")),
        check_vma=False,
    )
```
